32 devices in a mesh: groups: 2 (over y), pool: 8 (over z, x), heads: 2 (over core).
Axes of the slice: x: 2, y: 2, z: 4, core: 2. Of those that a mesh axis runs over, the one named last changes fastest.
Arguments:
- hidden_in: bfloat16 [32, 8192], P('groups'), parts along dimension 0, may hold values from -50 to 50
- key_cache: bfloat16 [32, 8, 4096, 128], P('groups', 'heads', 'pool'), parts along dimension 0, may hold values from -200 to 200
- value_cache: bfloat16 [32, 8, 4096, 128], P('groups', 'heads', 'pool'), parts along dimension 0, may hold values from -6 to 6
- positions: int32 [3, 32, 4096], P(None, 'groups', 'pool'), parts along dimension 1, may hold values from 0 to 4095, as said below
- query_pos: int32 [3, 32], P(None, 'groups'), parts along dimension 1, may hold values from 4096 to 8207
- lengths: int32 [32], P('groups'), parts along dimension 0, may hold values from 1024 to 4096, as said below
- query_weight: bfloat16 [8192, 8192], P('pool', 'heads'), may hold values from -0.0625 to 0.0625
- key_weight: bfloat16 [8192, 1024], P('pool', 'heads'), may hold values from -0.16503906 to 0.16503906
- value_weight: bfloat16 [8192, 1024], P('pool', 'heads'), may hold values from -0.16503906 to 0.16503906
- out_weight: bfloat16 [8192, 8192], P('heads', 'pool'), may hold values from -0.5 to 0.5
- gate_weight: bfloat16 [8192, 14848], P(None, ('pool', 'heads')), may hold values from -0.0625 to 0.0625
- up_weight: bfloat16 [8192, 14848], P(None, ('pool', 'heads')), may hold values from -0.0625 to 0.0625
- down_weight: bfloat16 [14848, 8192], P(('pool', 'heads')), may hold values from -0.0625 to 0.0625
Outputs:
- output: bfloat16 [32, 8192], P('groups', 'pool'), parts along dimension 0
The draws below stay inside these ranges and needn't reach their ends.
There are 2 independent parts, one for each index of `groups`. The reference program is written for one: setup_inputs(seed, part) draws one part's arguments, and reference() takes and returns one part's arrays. A program takes and returns all parts, laid end to end along the dimension named above; an argument that names none is the same for every part. Nothing has to cross between parts.
Inputs may be any that keep to these rules, and one draw needn't show every extreme that they name: `positions`: text tokens carry three equal ids; one prompt is text only. `lengths`: some prompt fills all 4096 slots.
All inputs are finite; a program needn't handle non-finite values.
Results may differ from the reference program's by a relative error of at most 0.007.
The reference program's roundings to bfloat16 on the way count: a program that leaves them out, or rounds other values in their place, can miss the bound.
Values may be sent and summed in bfloat16 or wider, within the bound.
No kernel may reach another device: no remote copies, remote signals or barrier semaphores. Data moves between devices by JAX's collectives and lax.ppermute only.
A program may use at most 192 MiB of HBM per device.

```python
import math
import jax
import jax.numpy as jnp
from jax import lax

D = 8192
HEADS = 64
KV_HEADS = 8
HD = 128
FF = 14848
PROMPTS = 16
SEQ = 4096


def draw_hidden_in(key, part):
    subkeys = jax.random.split(jax.random.fold_in(key, 11), 3)
    values_base = jax.random.truncated_normal(subkeys[0], -4.0, 4.0, (PROMPTS, D), jnp.float32)
    row_scale = jnp.exp(jax.random.uniform(subkeys[1], (PROMPTS, 1), jnp.float32, 0.0, math.log(4.0)))
    rise = math.log(10.0)
    column = jnp.arange(D).astype(jnp.float32) / D
    col_scale = jnp.exp(rise * (column - 0.5) + jax.random.uniform(subkeys[2], (D,), jnp.float32, -0.4, 0.4))
    return jnp.clip(values_base * row_scale * col_scale[None, :], -50.0, 50.0).astype(jnp.bfloat16)


def draw_key_cache(key, part):
    subkeys = jax.random.split(jax.random.fold_in(key, 53), 4)
    full_shape = (PROMPTS, KV_HEADS, SEQ, HD)
    base_values = 2.0 * jax.random.truncated_normal(subkeys[0], -6.0, 6.0, full_shape, jnp.float32)
    strength = jnp.exp(jax.random.uniform(subkeys[1], (PROMPTS, KV_HEADS, 1, 1), jnp.float32, math.log(30.0), math.log(200.0)))
    pattern = jax.random.rademacher(subkeys[2], (PROMPTS, KV_HEADS, 1, HD), jnp.float32)
    slot_choice = jax.random.randint(subkeys[3], (3, PROMPTS, KV_HEADS, 1, 1), 0, SEQ // 4)
    slot_index = jnp.arange(SEQ).reshape(1, 1, SEQ, 1)
    drawn = base_values
    for planted_index, factor in enumerate((1.0, 0.99, 0.98)):
        drawn = jnp.where(slot_index == slot_choice[planted_index], factor * strength * pattern, drawn)
    return jnp.clip(drawn, -200.0, 200.0).astype(jnp.bfloat16)


def draw_positions(key, part):
    subkeys = jax.random.split(jax.random.fold_in(key, 23), 3)
    text_len = jax.random.randint(subkeys[0], (PROMPTS,), 4, max(5, SEQ // 4))
    step_size = jax.random.randint(subkeys[1], (PROMPTS,), 1, 5)
    text_prompt = jax.random.randint(subkeys[2], (), 0, PROMPTS)
    token_index = jnp.arange(SEQ)[None, :]
    offset = token_index - text_len[:, None]
    in_video = (offset >= 0) & (jnp.arange(PROMPTS)[:, None] != text_prompt)
    clamped = jnp.maximum(offset, 0)
    frame = clamped // 64
    patch_row = clamped % 64 // 8
    patch_col = clamped % 8
    temporal = jnp.where(in_video, text_len[:, None] + frame * step_size[:, None], token_index)
    height = jnp.where(in_video, text_len[:, None] + patch_row, token_index)
    width = jnp.where(in_video, text_len[:, None] + patch_col, token_index)
    return jnp.clip(jnp.stack([temporal, height, width]), 0, SEQ - 1).astype(jnp.int32)


def draw_query_pos(key, part):
    subkeys = jax.random.split(jax.random.fold_in(key, 37), 2)
    anchor = jax.random.randint(subkeys[0], (1, PROMPTS), SEQ, 2 * SEQ)
    extra = jax.random.randint(subkeys[1], (3, PROMPTS), 0, 16)
    return (anchor + extra).astype(jnp.int32)


def draw_lengths(key, part):
    subkeys = jax.random.split(jax.random.fold_in(key, 41), 2)
    drawn = jax.random.randint(subkeys[0], (PROMPTS,), SEQ // 4, SEQ + 1)
    chosen = jax.random.randint(subkeys[1], (), 0, PROMPTS)
    return drawn.at[chosen].set(SEQ).astype(jnp.int32)


def spiked(values, rng, source, target, shards_of, factor):
    def block_of(axis_at):
        return (jnp.arange(values.shape[axis_at]) // (values.shape[axis_at] // shards_of)).reshape((-1,) + (1,) * (values.ndim - 1 - axis_at))

    one_side = jax.random.permutation(rng, shards_of)[block_of(target)]
    far = (block_of(target) + shards_of // 2) % shards_of
    return jnp.where((block_of(source) == one_side) | (block_of(source) == far), factor * values, values)


def block_levels(rng, shape, shards, low, high):
    gain, own = 1.0, jax.random.fold_in(rng, 6)
    for axis_at, shards_of in shards:
        draws = jnp.exp(jax.random.uniform(jax.random.fold_in(own, axis_at), (shards_of,), jnp.float32, low / len(shards), high / len(shards)))
        gain = gain * jnp.repeat(draws, shape[axis_at] // shards_of).reshape([-1 if axis == axis_at else 1 for axis in range(len(shape))])
    return gain


def centred(rng, dims, spread, most, shards=(), held_as=jnp.bfloat16):
    values = spread * jax.random.normal(rng, dims, jnp.float32)
    if shards:
        values = values * block_levels(rng, dims, shards, -0.22, 0.18)
    return jnp.clip(values, -most, most).astype(held_as)


def bell_draw_with(own_key, shape, spread, reach, shards, heavy, dtype=jnp.bfloat16):
    values = spread * jax.random.normal(own_key, shape, jnp.float32)
    if shards:
        values = values * block_levels(own_key, shape, shards, -0.22, 0.18)
    return jnp.clip(spiked(values, jax.random.fold_in(own_key, 3), *heavy), -reach, reach).astype(dtype)


def setup_inputs(seed: int = 0, part: int = 0) -> dict:
    arg_keys = jax.random.split(jax.random.key(seed), 14)
    part_keys = jax.random.split(jax.random.fold_in(arg_keys[13], part), 14)
    return {
        "hidden_in": draw_hidden_in(jax.random.fold_in(jax.random.fold_in(arg_keys[13], part), 71), part),
        "key_cache": draw_key_cache(jax.random.fold_in(jax.random.fold_in(arg_keys[13], part), 71), part),
        "value_cache": centred(part_keys[2], (PROMPTS, KV_HEADS, SEQ, HD), 1.0, 6.0, ((1, 2), (2, 8))),
        "positions": draw_positions(jax.random.fold_in(jax.random.fold_in(arg_keys[13], part), 71), part),
        "query_pos": draw_query_pos(jax.random.fold_in(jax.random.fold_in(arg_keys[13], part), 71), part),
        "lengths": draw_lengths(jax.random.fold_in(jax.random.fold_in(arg_keys[13], part), 71), part),
        "query_weight": centred(arg_keys[6], (D, HEADS * HD), D ** -0.5, 0.0625, ((0, 8), (1, 2))),
        "key_weight": centred(arg_keys[7], (D, KV_HEADS * HD), (2.5 / D ** 0.5), 0.16503906, ((0, 8), (1, 2))),
        "value_weight": centred(arg_keys[8], (D, KV_HEADS * HD), (2.5 / D ** 0.5), 0.16503906, ((0, 8), (1, 2))),
        "out_weight": centred(arg_keys[9], (HEADS * HD, D), HD ** -0.5, 0.5, ((0, 2), (1, 8))),
        "gate_weight": centred(arg_keys[10], (D, FF), D ** -0.5, 0.0625, ((1, 16),)),
        "up_weight": centred(arg_keys[11], (D, FF), D ** -0.5, 0.0625, ((1, 16),)),
        "down_weight": bell_draw_with(arg_keys[12], (FF, D), FF ** -0.5, 0.0625, ((0, 16),), (0, 1, 16, 2.0)),
    }


EPS = 1e-06
THETA = 1000000.0

def angle_tables(triple):
    half_dim = HD // 2
    column = jnp.arange(half_dim)
    first_end = HD // 8
    second_end = first_end + 3 * HD // 16
    chosen = jnp.where(column < first_end, triple[0][..., None], jnp.where(column < second_end, triple[1][..., None], triple[2][..., None]))
    inverse = jnp.exp(column.astype(jnp.float32) * (-2.0 * math.log(THETA) / HD))
    angles = chosen.astype(jnp.float32) * inverse
    return (jnp.cos(angles), jnp.sin(angles))

def rotate(values, cos_table, sin_table):
    half_dim = values.shape[-1] // 2
    lower_half = values[..., :half_dim]
    upper_half = values[..., half_dim:]
    return jnp.concatenate([lower_half * cos_table - upper_half * sin_table, upper_half * cos_table + lower_half * sin_table], -1)

def normalize(values):
    return values * lax.rsqrt(lax.optimization_barrier(jnp.mean(values * values, -1, keepdims=True)) + EPS)

def reference(hidden_in, key_cache, value_cache, positions, query_pos, lengths, query_weight, key_weight, value_weight, out_weight, gate_weight, up_weight, down_weight):
    group_size = HEADS // KV_HEADS
    score_scale = HD ** (-0.5)
    normed = normalize(hidden_in.astype(jnp.float32)).astype(jnp.bfloat16)
    raw_queries = jnp.dot(normed, query_weight, preferred_element_type=jnp.float32).reshape(PROMPTS, HEADS, HD)
    raw_keys = jnp.dot(normed, key_weight, preferred_element_type=jnp.float32).reshape(PROMPTS, KV_HEADS, HD)
    new_values = jnp.dot(normed, value_weight, preferred_element_type=jnp.float32).reshape(PROMPTS, KV_HEADS, HD).astype(jnp.bfloat16)
    query_cos, query_sin = angle_tables(query_pos)
    queries = rotate(raw_queries, query_cos[:, None], query_sin[:, None]).astype(jnp.bfloat16)
    own_keys = rotate(raw_keys, query_cos[:, None], query_sin[:, None]).astype(jnp.bfloat16)

    def attend_prompt(inputs):
        query_rows, key_new, value_new, cached_keys, cached_values, triple, length = inputs
        cos_table, sin_table = angle_tables(triple)
        rotated = rotate(cached_keys.astype(jnp.float32), cos_table[None], sin_table[None]).astype(jnp.bfloat16)
        grouped = query_rows.reshape(KV_HEADS, group_size, HD).astype(jnp.float32)
        scores = jnp.einsum('kgd,ksd->kgs', grouped, rotated.astype(jnp.float32)) * score_scale
        valid_mask = jnp.arange(SEQ) < length
        scores = jnp.where(valid_mask, scores, -1e+30)
        own_score = jnp.einsum('kgd,kd->kg', grouped, key_new.astype(jnp.float32)) * score_scale
        peak_score = jnp.maximum(lax.optimization_barrier(jnp.max(scores, -1)), own_score)
        weights = jnp.where(valid_mask, jnp.exp(scores - peak_score[..., None]), 0.0)
        own_weight = jnp.exp(own_score - peak_score)
        denominator = lax.optimization_barrier(jnp.sum(weights, -1)) + own_weight
        blended = jnp.einsum('kgs,ksd->kgd', weights, cached_values.astype(jnp.float32))
        blended = blended + own_weight[..., None] * value_new.astype(jnp.float32)[:, None, :]
        return (blended / denominator[..., None]).reshape(HEADS * HD).astype(jnp.bfloat16)
    triples = jnp.transpose(positions, (1, 0, 2))
    attended = lax.map(attend_prompt, (queries, own_keys, new_values, key_cache, value_cache, triples, lengths))
    attn_out = jnp.dot(attended, out_weight, preferred_element_type=jnp.float32)
    mid_state = (hidden_in.astype(jnp.float32) + attn_out).astype(jnp.bfloat16)
    normed_state = normalize(mid_state.astype(jnp.float32)).astype(jnp.bfloat16)
    gate_values = jnp.dot(normed_state, gate_weight, preferred_element_type=jnp.float32)
    up_values = jnp.dot(normed_state, up_weight, preferred_element_type=jnp.float32)
    active = (jax.nn.silu(gate_values) * up_values).astype(jnp.bfloat16)
    down_values = jnp.dot(active, down_weight, preferred_element_type=jnp.float32)
    return (mid_state.astype(jnp.float32) + down_values).astype(jnp.bfloat16)
```

```python
import math

import jax
import jax.numpy as jnp
from jax import lax
from jax.sharding import PartitionSpec as P

HD = 128
EPS = 1e-06
THETA = 1000000.0
NEG = -1e30


def sin_cos(angles):
    turns = (angles * (2.0 / math.pi) + 0.5).astype(jnp.int32)
    count = turns.astype(jnp.float32)
    rest = angles - count * 1.5703125
    rest = rest - count * 4.837512969970703125e-4
    rest = rest - count * 7.54978995489188216e-8
    square = rest * rest
    sine = ((-1.9515295891e-4 * square + 8.3321608736e-3) * square - 1.6666654611e-1) * square * rest + rest
    cosine = (
        ((2.443315711809948e-5 * square - 1.388731625493765e-3) * square + 4.166664568298827e-2) * square * square
        - 0.5 * square
        + 1.0
    )
    odd = (turns & 1) == 1
    sin_out = jnp.where(odd, cosine, sine)
    cos_out = jnp.where(odd, sine, cosine)
    sin_out = jnp.where((turns & 2) == 2, -sin_out, sin_out)
    cos_out = jnp.where(((turns + 1) & 2) == 2, -cos_out, cos_out)
    return sin_out, cos_out


def angle_tables(triple):
    half_dim = HD // 2
    column = jnp.arange(half_dim)
    first_end = HD // 8
    second_end = first_end + 3 * HD // 16
    chosen = jnp.where(
        column < first_end,
        triple[0][..., None],
        jnp.where(column < second_end, triple[1][..., None], triple[2][..., None]),
    )
    inverse = jnp.exp(column.astype(jnp.float32) * (-2.0 * math.log(THETA) / HD))
    sine, cosine = sin_cos(chosen.astype(jnp.float32) * inverse)
    return cosine, sine


def rotate(values, cos_table, sin_table):
    half_dim = values.shape[-1] // 2
    lower_half = values[..., :half_dim]
    upper_half = values[..., half_dim:]
    return jnp.concatenate(
        [
            lower_half * cos_table - upper_half * sin_table,
            upper_half * cos_table + lower_half * sin_table,
        ],
        -1,
    )


def exchange(pieces):
    return lax.all_to_all(pieces, "pool", 0, 0, tiled=True)


def gather(block):
    pool_size = lax.axis_size("pool")
    return exchange(jnp.broadcast_to(block[None], (pool_size,) + block.shape))


def heads_sum(values):
    size = lax.axis_size("heads")
    total = values
    moved = values
    for _ in range(size - 1):
        moved = lax.ppermute(moved, "heads", [(k, (k + 1) % size) for k in range(size)])
        total = total + moved
    return total


def per_device(
    hidden_in,
    key_cache,
    value_cache,
    positions,
    query_pos,
    lengths,
    query_weight,
    key_weight,
    value_weight,
    out_weight,
    gate_weight,
    up_weight,
    down_weight,
):
    pool_index = lax.axis_index("pool")
    pool_size = lax.axis_size("pool")
    prompts, width = hidden_in.shape
    local_heads, seq_local = key_cache.shape[1:3]
    query_width = query_weight.shape[1] // local_heads
    group_size = query_width // HD
    all_items = prompts * local_heads
    my_count = all_items // pool_size
    my_start = pool_index * my_count
    block_cols = width // pool_size
    scale = HD ** (-0.5)

    squares = jnp.sum(jnp.square(hidden_in.astype(jnp.float32)), -1, keepdims=True)
    hidden_cols = lax.dynamic_slice_in_dim(hidden_in, pool_index * block_cols, block_cols, 1)
    normed_cols = (hidden_cols.astype(jnp.float32) * lax.rsqrt(squares / width + EPS)).astype(jnp.bfloat16)
    term = jnp.concatenate(
        [
            jnp.dot(normed_cols, weight, preferred_element_type=jnp.float32).reshape(prompts, local_heads, -1)
            for weight in (query_weight, key_weight, value_weight)
        ],
        2,
    ).reshape(pool_size, my_count, query_width + 2 * HD)
    received = exchange(term)

    cos_table, sin_table = angle_tables(positions)
    rotated = rotate(key_cache.astype(jnp.float32), cos_table[:, None], sin_table[:, None]).astype(jnp.bfloat16)
    rotated = rotated.reshape(all_items, seq_local, HD)
    value_rows = value_cache.reshape(all_items, seq_local, HD)
    item_lengths = jnp.repeat(lengths, local_heads)

    projected = jnp.sum(received, 0).reshape(my_count, group_size + 2, HD)
    my_prompts = (my_start + jnp.arange(my_count)) // local_heads
    my_cos, my_sin = angle_tables(query_pos[:, my_prompts])
    turned = rotate(projected[:, : group_size + 1], my_cos[:, None], my_sin[:, None])
    mine = jnp.concatenate([turned, projected[:, group_size + 1 :]], 1).astype(jnp.bfloat16)
    everything = gather(mine).reshape(all_items, group_size + 2, HD)
    queries = everything[:, :group_size]
    own_keys = everything[:, group_size]
    own_values = everything[:, group_size + 1].astype(jnp.float32)

    scores = jnp.einsum("igd,isd->igs", queries, rotated, preferred_element_type=jnp.float32) * scale
    slot_index = pool_index * seq_local + jnp.arange(seq_local)
    valid_mask = slot_index[None, None, :] < item_lengths[:, None, None]
    scores = jnp.where(valid_mask, scores, NEG)
    own_score = jnp.einsum("igd,id->ig", queries, own_keys, preferred_element_type=jnp.float32) * scale
    own_score = jnp.where(pool_index == 0, own_score, NEG)
    peak = jnp.maximum(jnp.max(scores, -1), own_score)
    weights = jnp.where(valid_mask, jnp.exp(scores - peak[..., None]), 0.0)
    own_weight = jnp.where(pool_index == 0, jnp.exp(own_score - peak), 0.0)
    total = jnp.sum(weights, -1) + own_weight
    weighted = jnp.einsum("igs,isd->igd", weights, value_rows.astype(jnp.float32))
    weighted = weighted + own_weight[..., None] * own_values[:, None, :]
    safe_total = jnp.maximum(total, 1e-30)
    shares = (weighted / safe_total[..., None]).reshape(all_items, query_width)
    level = jnp.where(total > 0, peak + jnp.log(safe_total), NEG)
    first = lax.reduce_precision(level, 8, 7)
    second = lax.reduce_precision(level - first, 8, 7)
    third = level - first - second
    packed = jnp.concatenate([shares, first, second, third], 1).astype(jnp.bfloat16)
    parts = gather(packed).astype(jnp.float32)
    levels = parts[..., query_width:].reshape(pool_size, all_items, 3, group_size)
    levels = levels[:, :, 0] + levels[:, :, 1] + levels[:, :, 2]
    factor = jnp.exp(levels - jnp.max(levels, 0))
    factor = factor / jnp.sum(factor, 0)
    shares = parts[..., :query_width].reshape(pool_size, all_items, group_size, HD)
    attended = jnp.sum(shares * factor[..., None], 0).astype(jnp.bfloat16)
    attended = attended.reshape(prompts, local_heads * query_width)

    attn_out = heads_sum(jnp.dot(attended, out_weight, preferred_element_type=jnp.float32))
    mid_state = (hidden_cols.astype(jnp.float32) + attn_out).astype(jnp.bfloat16)
    whole_state = gather(mid_state).transpose(1, 0, 2).reshape(prompts, width).astype(jnp.float32)
    inverse = lax.rsqrt(jnp.mean(jnp.square(whole_state), -1, keepdims=True) + EPS)
    normed_state = (whole_state * inverse).astype(jnp.bfloat16)
    gate_values = jnp.dot(normed_state, gate_weight, preferred_element_type=jnp.float32)
    up_values = jnp.dot(normed_state, up_weight, preferred_element_type=jnp.float32)
    active = (jax.nn.silu(gate_values) * up_values).astype(jnp.bfloat16)
    partial_out = jnp.dot(active, down_weight, preferred_element_type=jnp.float32).astype(jnp.bfloat16)
    pieces = exchange(partial_out.reshape(prompts, pool_size, block_cols).transpose(1, 0, 2))
    mlp_cols = heads_sum(jnp.sum(pieces.astype(jnp.float32), 0))
    return (mid_state.astype(jnp.float32) + mlp_cols).astype(jnp.bfloat16)


def solution(mesh):
    in_specs = (
        P("groups", None),
        P("groups", "heads", "pool", None),
        P("groups", "heads", "pool", None),
        P(None, "groups", "pool"),
        P(None, "groups"),
        P("groups"),
        P("pool", "heads"),
        P("pool", "heads"),
        P("pool", "heads"),
        P("heads", "pool"),
        P(None, ("pool", "heads")),
        P(None, ("pool", "heads")),
        P(("pool", "heads"), None),
    )
    out_specs = P("groups", "pool")
    return jax.shard_map(per_device, mesh=mesh, in_specs=in_specs, out_specs=out_specs, check_vma=False)
```

```python
import math

import jax
import jax.numpy as jnp
from jax import lax
from jax.experimental import pallas as pl
from jax.experimental.pallas import tpu as pltpu
from jax.sharding import PartitionSpec as P

HD = 128
EPS = 1e-06
THETA = 1000000.0
NEG = -1e30


def sin_cos(angles):
    turns = (angles * (2.0 / math.pi) + 0.5).astype(jnp.int32)
    count = turns.astype(jnp.float32)
    rest = angles - count * 1.5703125
    rest = rest - count * 4.837512969970703125e-4
    rest = rest - count * 7.54978995489188216e-8
    square = rest * rest
    sine = ((-1.9515295891e-4 * square + 8.3321608736e-3) * square - 1.6666654611e-1) * square * rest + rest
    cosine = (
        ((2.443315711809948e-5 * square - 1.388731625493765e-3) * square + 4.166664568298827e-2) * square * square
        - 0.5 * square
        + 1.0
    )
    odd = (turns & 1) == 1
    sin_out = jnp.where(odd, cosine, sine)
    cos_out = jnp.where(odd, sine, cosine)
    sin_out = jnp.where((turns & 2) == 2, -sin_out, sin_out)
    cos_out = jnp.where(((turns + 1) & 2) == 2, -cos_out, cos_out)
    return sin_out, cos_out


def frequencies():
    column = jnp.arange(HD // 2)
    return jnp.exp(column.astype(jnp.float32) * (-2.0 * math.log(THETA) / HD))


def sections():
    first_end = HD // 8
    second_end = first_end + 3 * HD // 16
    column = jnp.arange(HD // 2)
    return (column >= first_end).astype(jnp.int32) + (column >= second_end).astype(jnp.int32)


def small_grant(mebibytes):
    return pltpu.CompilerParams(vmem_limit_bytes=mebibytes << 20)


def rope_keys(key_cache, positions):
    prompts, heads, slots, _ = key_cache.shape
    pairs = prompts // 2
    low_bits = 64
    halves = positions.reshape(3, 2, pairs, slots)
    digits = jnp.stack([halves // low_bits, halves % low_bits], 1)
    digits = jnp.pad(digits.transpose(3, 2, 1, 0, 4).reshape(pairs, 2, 6, slots), ((0, 0), (0, 0), (0, 2), (0, 0)))
    digits = digits.reshape(pairs, 16, slots).astype(jnp.bfloat16)
    one_hot = (sections()[None, :] == jnp.arange(3)[:, None]).astype(jnp.float32)
    one_hot = jnp.concatenate([one_hot * low_bits, one_hot, jnp.zeros((2, HD // 2))], 0)
    blank = jnp.zeros_like(one_hot)
    picker = jnp.concatenate(
        [jnp.concatenate([one_hot, blank], 1), jnp.concatenate([blank, one_hot], 1)], 0
    ).astype(jnp.bfloat16)
    inverse = jnp.tile(frequencies(), 2)[None]
    chunk = min(slots, 64)

    def body(digits_ref, picker_ref, inverse_ref, key_ref, out_ref, *table_refs):
        chosen = lax.dot_general(
            digits_ref[0], picker_ref[...], (((0,), (0,)), ((), ())), preferred_element_type=jnp.float32
        )
        first = lax.broadcasted_iota(jnp.int32, (chunk, HD), 1) < HD // 2
        for start in range(0, slots, chunk):
            rows = slice(start, start + chunk)
            sine, cosine = sin_cos(chosen[rows] * inverse_ref[...])
            cosine_rolled = pltpu.roll(cosine, HD // 2, 1)
            sine_rolled = pltpu.roll(sine, HD // 2, 1)
            table_refs[0][0, rows, :] = jnp.where(first, cosine, cosine_rolled)
            table_refs[0][1, rows, :] = jnp.where(first, cosine_rolled, cosine)
            table_refs[1][0, rows, :] = jnp.where(first, -sine, sine_rolled)
            table_refs[1][1, rows, :] = jnp.where(first, -sine_rolled, sine)
        for half in range(2):
            for start in range(0, slots, chunk):
                rows = slice(start, start + chunk)
                cos_rows = table_refs[0][half, rows, :]
                sin_rows = table_refs[1][half, rows, :]
                for head in range(heads):
                    keys = key_ref[half, 0, head, rows, :].astype(jnp.float32)
                    turned = keys * cos_rows + pltpu.roll(keys, HD // 2, 1) * sin_rows
                    out_ref[half, 0, head, rows, :] = turned.astype(jnp.bfloat16)

    shape = (2, pairs, heads, slots, HD)
    block = pl.BlockSpec((2, 1, heads, slots, HD), lambda i: (0, i, 0, 0, 0))
    rotated = pl.pallas_call(
        body,
        grid=(pairs,),
        in_specs=[
            pl.BlockSpec((1, 16, slots), lambda i: (i, 0, 0)),
            pl.BlockSpec((16, HD), lambda i: (0, 0)),
            pl.BlockSpec((1, HD), lambda i: (0, 0)),
            block,
        ],
        out_specs=block,
        out_shape=jax.ShapeDtypeStruct(shape, jnp.bfloat16),
        scratch_shapes=[pltpu.VMEM((2, slots, HD), jnp.float32)] * 2,
        compiler_params=small_grant(60),
        name="rope_keys",
    )(digits, picker, inverse, key_cache.reshape(shape))
    return rotated.reshape(prompts * heads, slots, HD)


def finish_rows(received, cos_rows, sin_rows):
    pool_size, rows, _ = received.shape

    def body(received_ref, cos_ref, sin_ref, out_ref):
        total = received_ref[0]
        for source in range(1, pool_size):
            total = total + received_ref[source]
        turned = total * cos_ref[...] + pltpu.roll(total, HD // 2, 1) * sin_ref[...]
        turned = turned.astype(jnp.bfloat16)
        for target in range(pool_size):
            out_ref[target] = turned

    return pl.pallas_call(
        body, out_shape=jax.ShapeDtypeStruct((pool_size, rows, HD), jnp.bfloat16), name="finish_rows",
        compiler_params=small_grant(4),
    )(received, cos_rows, sin_rows)


def attend(info, new_rows, rotated, values, local_heads, group_size):
    pool_size = new_rows.shape[0]
    all_items, slots, _ = rotated.shape
    my_count = all_items // pool_size
    pair = 2 if my_count % 2 == 0 else 1
    rows = pair * group_size
    query_rows = my_count * group_size
    scale = HD ** (-0.5)
    prompts = all_items // local_heads

    groups = [[first + k for k in range(pair)] for first in range(0, my_count, pair)]

    def body(info_ref, new_ref, key_ref, value_ref, out_ref):
        block = pl.program_id(0)
        row_index = lax.broadcasted_iota(jnp.int32, (rows, 1), 0)
        slot_index = lax.broadcasted_iota(jnp.int32, (query_rows, slots), 1)
        lane = lax.broadcasted_iota(jnp.int32, (rows, HD), 1)
        holds_own = info_ref[prompts] == 0
        in_item = [row_index // group_size == k for k in range(pair)]

        def spread(piece, width):
            return jnp.concatenate(
                [jnp.broadcast_to(piece(item), (group_size, width)) for item in range(my_count)], 0
            )

        queries = new_ref[0, :query_rows, :].astype(jnp.float32)
        own_rows = new_ref[0, query_rows:, :].astype(jnp.float32)
        scores = []
        for index, items in enumerate(groups):
            part = queries[index * rows : (index + 1) * rows]
            wide_queries = jnp.concatenate([jnp.where(mask, part, 0.0).astype(jnp.bfloat16) for mask in in_item], 1)
            wide_keys = jnp.concatenate([key_ref[item] for item in items], 1)
            scores.append(
                lax.dot_general(
                    wide_queries, wide_keys, (((1,), (1,)), ((), ())), preferred_element_type=jnp.float32
                )
            )
        scores = jnp.concatenate(scores, 0) * scale
        limits = spread(lambda item: jnp.full((1, 1), info_ref[(block * my_count + item) // local_heads]), 1)
        valid = slot_index < limits
        scores = jnp.where(valid, scores, NEG)
        own_keys = spread(lambda item: own_rows[item : item + 1], HD)
        own_values = spread(lambda item: own_rows[my_count + item : my_count + item + 1], HD)
        own_score = jnp.sum(queries * own_keys, 1, keepdims=True) * scale
        own_score = jnp.where(holds_own, own_score, NEG)
        peak = jnp.maximum(jnp.max(scores, 1, keepdims=True), own_score)
        weights = jnp.where(valid, jnp.exp(scores - peak), 0.0)
        own_weight = jnp.where(holds_own, jnp.exp(own_score - peak), 0.0)
        total = jnp.sum(weights, 1, keepdims=True) + own_weight
        coarse = weights.astype(jnp.bfloat16)
        fine = (weights - coarse.astype(jnp.float32)).astype(jnp.bfloat16)
        blended = []
        for index, items in enumerate(groups):
            span = slice(index * rows, (index + 1) * rows)
            wide_values = jnp.concatenate([value_ref[item] for item in items], 1)
            both = jnp.dot(
                jnp.concatenate([coarse[span], fine[span]], 0), wide_values, preferred_element_type=jnp.float32
            )
            both = both[:rows] + both[rows:]
            chosen = both[:, :HD]
            for k in range(1, pair):
                chosen = jnp.where(in_item[k], both[:, k * HD : (k + 1) * HD], chosen)
            blended.append(chosen)
        blended = jnp.concatenate(blended, 0) + own_weight * own_values
        safe_total = jnp.maximum(total, 1e-30)
        out_ref[0, :query_rows, :] = (blended / safe_total).astype(jnp.bfloat16)
        level = jnp.where(total > 0, peak + jnp.log(safe_total), NEG)
        stamp = jnp.zeros((rows, HD), jnp.float32)
        for part in range(3):
            rounded = level.astype(jnp.bfloat16).astype(jnp.float32)
            level = level - rounded
            for index in range(len(groups)):
                stamp = jnp.where(lane == index * 3 + part, rounded[index * rows : (index + 1) * rows], stamp)
        out_ref[0, query_rows:, :] = stamp.astype(jnp.bfloat16)

    cache_block = pl.BlockSpec((my_count, slots, HD), lambda i, info: (i, 0, 0))
    return pl.pallas_call(
        body,
        grid_spec=pltpu.PrefetchScalarGridSpec(
            num_scalar_prefetch=1,
            grid=(pool_size,),
            in_specs=[
                pl.BlockSpec((1,) + new_rows.shape[1:], lambda i, info: (i, 0, 0)),
                cache_block,
                cache_block,
            ],
            out_specs=pl.BlockSpec((1, query_rows + rows, HD), lambda i, info: (i, 0, 0)),
        ),
        out_shape=jax.ShapeDtypeStruct((pool_size, query_rows + rows, HD), jnp.bfloat16),
        name="attend",
        compiler_params=small_grant(60),
    )(info, new_rows, rotated, values)


def combine(parts, my_count, group_size):
    pool_size = parts.shape[0]
    pair = 2 if my_count % 2 == 0 else 1
    rows = pair * group_size
    query_rows = my_count * group_size

    def body(parts_ref, out_ref):
        lane = lax.broadcasted_iota(jnp.int32, (rows, HD), 1)
        stamps = [parts_ref[source, query_rows:, :].astype(jnp.float32) for source in range(pool_size)]
        for group in range(my_count // pair):
            in_group = (lane >= group * 3) & (lane < group * 3 + 3)
            levels = [jnp.sum(jnp.where(in_group, stamp, 0.0), 1, keepdims=True) for stamp in stamps]
            top = levels[0]
            for level in levels[1:]:
                top = jnp.maximum(top, level)
            factors = [jnp.exp(level - top) for level in levels]
            whole = factors[0]
            for factor in factors[1:]:
                whole = whole + factor
            span = slice(group * rows, (group + 1) * rows)
            blended = jnp.zeros((rows, HD), jnp.float32)
            for source in range(pool_size):
                blended = blended + parts_ref[source, span, :].astype(jnp.float32) * factors[source]
            blended = (blended / whole).astype(jnp.bfloat16)
            for target in range(pool_size):
                out_ref[target, span, :] = blended

    return pl.pallas_call(
        body, out_shape=jax.ShapeDtypeStruct((pool_size, query_rows, HD), jnp.bfloat16), name="combine",
        compiler_params=small_grant(4),
    )(parts)


def feed_forward(state, gate_weight, up_weight, down_weight):
    pool_size, prompts, block_cols = state.shape
    width = pool_size * block_cols
    hidden = gate_weight.shape[1]
    across = (((1,), (1,)), ((), ()))

    def body(state_ref, gate_hbm, up_hbm, down_hbm, out_ref, gate_ref, up_ref, down_ref, sems):
        spans = [slice(k * block_cols, (k + 1) * block_cols) for k in range(pool_size)]
        copies = []
        for index, span in enumerate(spans):
            for which, (source, target) in enumerate(((gate_hbm, gate_ref), (up_hbm, up_ref), (down_hbm, down_ref))):
                copies.append(pltpu.make_async_copy(source.at[:, span], target.at[:, span], sems.at[which, index]))
        for index in range(pool_size):
            copies[3 * index].start()
            copies[3 * index + 1].start()
        for index in range(pool_size):
            copies[3 * index + 2].start()
        squares = jnp.zeros((prompts, 1), jnp.float32)
        for source in range(pool_size):
            rows = state_ref[source].astype(jnp.float32)
            squares = squares + jnp.sum(rows * rows, 1, keepdims=True)
        inverse = lax.rsqrt(squares / width + EPS)
        gate_values = jnp.zeros((prompts, hidden), jnp.float32)
        up_values = jnp.zeros((prompts, hidden), jnp.float32)
        for index, span in enumerate(spans):
            rows = (state_ref[index].astype(jnp.float32) * inverse).astype(jnp.bfloat16)
            copies[3 * index].wait()
            gate_values = gate_values + lax.dot_general(
                rows, gate_ref[:, span], across, preferred_element_type=jnp.float32
            )
            copies[3 * index + 1].wait()
            up_values = up_values + lax.dot_general(
                rows, up_ref[:, span], across, preferred_element_type=jnp.float32
            )
        active = (gate_values / (1.0 + jnp.exp(-gate_values)) * up_values).astype(jnp.bfloat16)
        for index, span in enumerate(spans):
            copies[3 * index + 2].wait()
            out_ref[index] = jnp.dot(active, down_ref[:, span], preferred_element_type=jnp.float32).astype(
                jnp.bfloat16
            )

    whole = pl.BlockSpec(memory_space=pltpu.VMEM)
    return pl.pallas_call(
        body,
        in_specs=[whole] + [pl.BlockSpec(memory_space=pltpu.HBM)] * 3,
        scratch_shapes=[
            pltpu.VMEM((hidden, width), gate_weight.dtype),
            pltpu.VMEM((hidden, width), up_weight.dtype),
            pltpu.VMEM((hidden, width), down_weight.dtype),
            pltpu.SemaphoreType.DMA((3, pool_size)),
        ],
        out_shape=jax.ShapeDtypeStruct(state.shape, jnp.bfloat16),
        name="feed_forward",
        compiler_params=small_grant(60),
        cost_estimate=pl.CostEstimate(
            flops=6 * prompts * width * hidden, bytes_accessed=6 * width * hidden, transcendentals=prompts * hidden
        ),
    )(state, gate_weight.T, up_weight.T, down_weight)


def exchange(pieces):
    return lax.all_to_all(pieces, "pool", 0, 0, tiled=True)


def gather(block):
    pool_size = lax.axis_size("pool")
    return exchange(jnp.broadcast_to(block[None], (pool_size,) + block.shape))


def heads_sum(values):
    size = lax.axis_size("heads")
    total = values
    moved = values
    for _ in range(size - 1):
        moved = lax.ppermute(moved, "heads", [(k, (k + 1) % size) for k in range(size)])
        total = total + moved
    return total


def per_device(
    hidden_in,
    key_cache,
    value_cache,
    positions,
    query_pos,
    lengths,
    query_weight,
    key_weight,
    value_weight,
    out_weight,
    gate_weight,
    up_weight,
    down_weight,
):
    pool_index = lax.axis_index("pool")
    pool_size = lax.axis_size("pool")
    prompts, width = hidden_in.shape
    local_heads, seq_local = key_cache.shape[1:3]
    query_width = query_weight.shape[1] // local_heads
    group_size = query_width // HD
    all_items = prompts * local_heads
    my_count = all_items // pool_size
    my_start = pool_index * my_count
    block_cols = width // pool_size

    squares = jnp.sum(jnp.square(hidden_in.astype(jnp.float32)), -1, keepdims=True)
    hidden_cols = lax.dynamic_slice_in_dim(hidden_in, pool_index * block_cols, block_cols, 1)
    normed_cols = (hidden_cols.astype(jnp.float32) * lax.rsqrt(squares / width + EPS)).astype(jnp.bfloat16)
    projected = [
        jnp.dot(normed_cols, weight, preferred_element_type=jnp.float32).reshape(pool_size, -1, HD)
        for weight in (query_weight, key_weight, value_weight)
    ]
    info = jnp.concatenate([lengths - pool_index * seq_local, jnp.full((1,), pool_index, jnp.int32)])
    projected, info = lax.optimization_barrier((jnp.concatenate(projected, 1), info))
    received = exchange(projected)

    rotated = rope_keys(key_cache, positions)
    value_rows = value_cache.reshape(all_items, seq_local, HD)
    row_items = my_start + jnp.concatenate(
        [jnp.repeat(jnp.arange(my_count), group_size), jnp.arange(my_count), jnp.arange(my_count)]
    )
    row_prompts = row_items // local_heads
    turning = (jnp.arange(my_count * (group_size + 2)) < my_count * (group_size + 1))[:, None]
    picked = (row_prompts[:, None] == jnp.arange(prompts)) & turning
    section = sections()
    chosen = jnp.zeros((row_items.shape[0], HD // 2), jnp.int32)
    for axis in range(3):
        ids = jnp.sum(jnp.where(picked, query_pos[axis][None], 0), 1)
        chosen = jnp.where(section == axis, ids[:, None], chosen)
    sine, cosine = sin_cos(chosen.astype(jnp.float32) * frequencies())
    cos_rows = jnp.concatenate([cosine, cosine], 1)
    sin_rows = jnp.concatenate([-sine, sine], 1)
    received, rotated = lax.optimization_barrier((received, rotated))
    new_rows = exchange(finish_rows(received, cos_rows, sin_rows))

    parts = exchange(attend(info, new_rows, rotated, value_rows, local_heads, group_size))
    attended = exchange(combine(parts, my_count, group_size))
    attended = attended.reshape(prompts, local_heads * query_width)

    attn_out = heads_sum(jnp.dot(attended, out_weight, preferred_element_type=jnp.float32))
    mid_state = (hidden_cols.astype(jnp.float32) + attn_out).astype(jnp.bfloat16)
    pieces = exchange(feed_forward(gather(mid_state), gate_weight, up_weight, down_weight))
    mlp_cols = heads_sum(jnp.sum(pieces.astype(jnp.float32), 0))
    return (mid_state.astype(jnp.float32) + mlp_cols).astype(jnp.bfloat16)


def solution(mesh):
    in_specs = (
        P("groups", None),
        P("groups", "heads", "pool", None),
        P("groups", "heads", "pool", None),
        P(None, "groups", "pool"),
        P(None, "groups"),
        P("groups"),
        P("pool", "heads"),
        P("pool", "heads"),
        P("pool", "heads"),
        P("heads", "pool"),
        P(None, ("pool", "heads")),
        P(None, ("pool", "heads")),
        P(("pool", "heads"), None),
    )
    out_specs = P("groups", "pool")
    return jax.shard_map(per_device, mesh=mesh, in_specs=in_specs, out_specs=out_specs, check_vma=False)
```

```python
import math

import jax
import jax.numpy as jnp
from jax import lax
from jax.experimental import pallas as pl
from jax.experimental.pallas import tpu as pltpu
from jax.sharding import PartitionSpec as P

HD = 128
EPS = 1e-06
THETA = 1000000.0
NEG = -1e30


def sin_cos(angles):
    turns = (angles * (2.0 / math.pi) + 0.5).astype(jnp.int32)
    count = turns.astype(jnp.float32)
    rest = angles - count * 1.5703125
    rest = rest - count * 4.837512969970703125e-4
    rest = rest - count * 7.54978995489188216e-8
    square = rest * rest
    sine = ((-1.9515295891e-4 * square + 8.3321608736e-3) * square - 1.6666654611e-1) * square * rest + rest
    cosine = (
        ((2.443315711809948e-5 * square - 1.388731625493765e-3) * square + 4.166664568298827e-2) * square * square
        - 0.5 * square
        + 1.0
    )
    odd = (turns & 1) == 1
    sin_out = jnp.where(odd, cosine, sine)
    cos_out = jnp.where(odd, sine, cosine)
    sin_out = jnp.where((turns & 2) == 2, -sin_out, sin_out)
    cos_out = jnp.where(((turns + 1) & 2) == 2, -cos_out, cos_out)
    return sin_out, cos_out


def frequencies():
    column = jnp.arange(HD // 2)
    return jnp.exp(column.astype(jnp.float32) * (-2.0 * math.log(THETA) / HD))


def sections():
    first_end = HD // 8
    second_end = first_end + 3 * HD // 16
    column = jnp.arange(HD // 2)
    return (column >= first_end).astype(jnp.int32) + (column >= second_end).astype(jnp.int32)


def small_grant(mebibytes):
    return pltpu.CompilerParams(vmem_limit_bytes=mebibytes << 20)


def rope_keys(key_cache, positions, first_pair, last_pair, partner):
    _, pairs, heads, slots, _ = key_cache.shape
    low_bits = 6
    chunk = min(slots, 64)
    count = last_pair - first_pair
    inverse = jnp.tile(frequencies(), 2)[None]

    def body(positions_ref, inverse_ref, key_hbm, *refs):
        out_hbm, key_ref, out_ref, chosen_ref, cos_ref, sin_ref, sems = refs[-7:]

        def copy_in(index):
            return pltpu.make_async_copy(key_hbm.at[:, first_pair + index], key_ref.at[:, index], sems.at[0, index])

        def copy_out(index):
            return pltpu.make_async_copy(out_ref.at[:, index], out_hbm.at[:, first_pair + index], sems.at[1, index])

        for index in range(count):
            copy_in(index).start()
        first = lax.broadcasted_iota(jnp.int32, (chunk, HD), 1) < HD // 2
        row = lax.broadcasted_iota(jnp.int32, (16, HD), 0)
        lane = lax.broadcasted_iota(jnp.int32, (16, HD), 1)
        column = lane % (HD // 2)
        first_end = HD // 8
        section = (column >= first_end).astype(jnp.int32) + (column >= first_end + 3 * HD // 16).astype(jnp.int32)
        within = row % 8
        own_half = row // 8 == lane // (HD // 2)
        picker = jnp.where(own_half & (within == section), float(1 << low_bits), 0.0)
        picker = jnp.where(own_half & (within == section + 3), 1.0, picker).astype(jnp.bfloat16)
        blank = jnp.zeros((2, slots), jnp.float32)

        def step(index, carry):
            digits = []
            for half in range(2):
                ids = [positions_ref[axis, pl.ds(half * pairs + first_pair + index, 1), :] for axis in range(3)]
                digits += [(value >> low_bits).astype(jnp.float32) for value in ids]
                digits += [(value & ((1 << low_bits) - 1)).astype(jnp.float32) for value in ids]
                digits.append(blank)
            chosen_ref[...] = lax.dot_general(
                jnp.concatenate(digits, 0).astype(jnp.bfloat16),
                picker,
                (((0,), (0,)), ((), ())),
                preferred_element_type=jnp.float32,
            )
            for start in range(0, slots, chunk):
                rows = slice(start, start + chunk)
                sine, cosine = sin_cos(chosen_ref[rows, :] * inverse_ref[...])
                cosine_rolled = pltpu.roll(cosine, HD // 2, 1)
                sine_rolled = pltpu.roll(sine, HD // 2, 1)
                cos_ref[0, rows, :] = jnp.where(first, cosine, cosine_rolled)
                cos_ref[1, rows, :] = jnp.where(first, cosine_rolled, cosine)
                sin_ref[0, rows, :] = jnp.where(first, -sine, sine_rolled)
                sin_ref[1, rows, :] = jnp.where(first, -sine_rolled, sine)
            copy_in(index).wait()
            for half in range(2):
                for start in range(0, slots, chunk):
                    rows = slice(start, start + chunk)
                    cos_rows = cos_ref[half, rows, :]
                    sin_rows = sin_ref[half, rows, :]
                    for head in range(heads):
                        keys = key_ref[half, index, head, rows, :].astype(jnp.float32)
                        turned = keys * cos_rows + pltpu.roll(keys, HD // 2, 1) * sin_rows
                        out_ref[half, index, head, rows, :] = turned.astype(jnp.bfloat16)
            copy_out(index).start()
            return carry

        lax.fori_loop(0, count, step, 0)
        for index in range(count):
            copy_out(index).wait()

    vmem = pl.BlockSpec(memory_space=pltpu.VMEM)
    hbm = pl.BlockSpec(memory_space=pltpu.HBM)
    partners = () if partner is None else (partner,)
    return pl.pallas_call(
        body,
        in_specs=[vmem, vmem, hbm] + [hbm for _ in partners],
        out_specs=hbm,
        out_shape=jax.ShapeDtypeStruct(key_cache.shape, jnp.bfloat16),
        input_output_aliases={3: 0} if partners else {},
        scratch_shapes=[
            pltpu.VMEM((2, count) + key_cache.shape[2:], jnp.bfloat16),
            pltpu.VMEM((2, count) + key_cache.shape[2:], jnp.bfloat16),
            pltpu.VMEM((slots, HD), jnp.float32),
            pltpu.VMEM((2, slots, HD), jnp.float32),
            pltpu.VMEM((2, slots, HD), jnp.float32),
            pltpu.SemaphoreType.DMA((2, count)),
        ],
        compiler_params=small_grant(56),
        name="rope_keys",
    )(positions, inverse, key_cache, *partners)


def project(hidden_in, weights, pool_size, local_heads, group_size):
    prompts, width = hidden_in.shape
    block_cols = width // pool_size
    my_count = prompts * local_heads // pool_size
    rows = my_count * (group_size + 2)
    columns = [weight.shape[1] for weight in weights]
    query_columns = columns[0]
    pieces = max(1, min(8, query_columns // 512))
    piece = query_columns // pieces

    def place(kind, head, group):
        if kind == 0:
            return lambda item: item * group_size + group
        return lambda item: my_count * (group_size + kind - 1) + item

    def body(hidden_ref, query_hbm, key_hbm, value_hbm, out_ref, query_ref, key_ref, value_ref, flat_ref, sems):
        copies = []
        for index in range(pieces):
            span = slice(index * piece, (index + 1) * piece)
            copies.append(pltpu.make_async_copy(query_hbm.at[:, span], query_ref.at[:, span], sems.at[index]))
        copies.append(pltpu.make_async_copy(key_hbm, key_ref, sems.at[pieces]))
        copies.append(pltpu.make_async_copy(value_hbm, value_ref, sems.at[pieces + 1]))
        for copy in copies:
            copy.start()
        hidden = hidden_ref[...].astype(jnp.float32)
        squares = jnp.sum(hidden * hidden, 1, keepdims=True)
        start = pl.multiple_of(lax.axis_index("pool") * block_cols, block_cols)
        mine = hidden_ref[:, pl.ds(start, block_cols)].astype(jnp.float32)
        normed = (mine * lax.rsqrt(squares / width + EPS)).astype(jnp.bfloat16)

        def spread(kind, first_block, count, values):
            for offset in range(count):
                flat_ref[offset * prompts : (offset + 1) * prompts, :] = values[:, offset * HD : (offset + 1) * HD]
                number = first_block + offset
                head, group = (number // group_size, number % group_size) if kind == 0 else (number, 0)
                row_of = place(kind, head, group)
                if my_count >= local_heads:
                    per_device = my_count // local_heads
                    for turn in range(per_device):
                        out_ref[pl.ds(row_of(turn * local_heads + head), pool_size, stride=rows), :] = flat_ref[
                            pl.ds(offset * prompts + turn, pool_size, stride=per_device), :
                        ]
                else:
                    split = local_heads // my_count
                    base = (head // my_count) * rows + row_of(head % my_count)
                    out_ref[pl.ds(base, prompts, stride=split * rows), :] = flat_ref[
                        offset * prompts : (offset + 1) * prompts, :
                    ]

        for index in range(pieces):
            span = slice(index * piece, (index + 1) * piece)
            copies[index].wait()
            values = jnp.dot(normed, query_ref[:, span], preferred_element_type=jnp.float32)
            spread(0, index * (piece // HD), piece // HD, values)
        for kind, ref in ((1, key_ref), (2, value_ref)):
            copies[pieces + kind - 1].wait()
            values = jnp.dot(normed, ref[...], preferred_element_type=jnp.float32)
            spread(kind, 0, local_heads, values)

    vmem = pl.BlockSpec(memory_space=pltpu.VMEM)
    hbm = pl.BlockSpec(memory_space=pltpu.HBM)
    out = pl.pallas_call(
        body,
        in_specs=[vmem, hbm, hbm, hbm],
        out_specs=vmem,
        out_shape=jax.ShapeDtypeStruct((pool_size * rows, HD), jnp.float32),
        scratch_shapes=[pltpu.VMEM(weight.shape, weight.dtype) for weight in weights]
        + [
            pltpu.VMEM((prompts * max(piece // HD, local_heads), HD), jnp.float32),
            pltpu.SemaphoreType.DMA((pieces + 2,)),
        ],
        compiler_params=small_grant(56),
        name="project",
    )(hidden_in, *weights)
    return out.reshape(pool_size, rows, HD)


def project_out(attended, out_weight, prompts):
    total_rows = attended.shape[0] * attended.shape[1]
    blocks = total_rows // prompts
    attended = attended.reshape(total_rows, HD)
    pieces = max(1, min(8, blocks // 2))
    per_piece = blocks // pieces
    depth = per_piece * HD

    def body(attended_ref, weight_hbm, out_ref, weight_ref, wide_ref, sems):
        copies = []
        for index in range(pieces):
            span = slice(index * depth, (index + 1) * depth)
            copies.append(pltpu.make_async_copy(weight_hbm.at[span], weight_ref.at[span], sems.at[index]))
            copies[-1].start()
        wide_ref[...] = attended_ref[...].astype(jnp.float32)
        total = jnp.zeros(out_ref.shape, jnp.float32)
        for index in range(pieces):
            rows = [
                wide_ref[pl.ds(index * per_piece + k, prompts, stride=blocks), :].astype(jnp.bfloat16)
                for k in range(per_piece)
            ]
            copies[index].wait()
            total = total + jnp.dot(
                jnp.concatenate(rows, 1),
                weight_ref[index * depth : (index + 1) * depth, :],
                preferred_element_type=jnp.float32,
            )
        out_ref[...] = total

    vmem = pl.BlockSpec(memory_space=pltpu.VMEM)
    return pl.pallas_call(
        body,
        in_specs=[vmem, pl.BlockSpec(memory_space=pltpu.HBM)],
        out_specs=vmem,
        out_shape=jax.ShapeDtypeStruct((prompts, out_weight.shape[1]), jnp.float32),
        scratch_shapes=[
            pltpu.VMEM(out_weight.shape, out_weight.dtype),
            pltpu.VMEM((total_rows, HD), jnp.float32),
            pltpu.SemaphoreType.DMA((pieces,)),
        ],
        compiler_params=small_grant(53),
        name="project_out",
    )(attended, out_weight)


def finish_rows(received, cos_rows, sin_rows):
    pool_size, rows, _ = received.shape

    def body(received_ref, cos_ref, sin_ref, out_ref):
        total = received_ref[0]
        for source in range(1, pool_size):
            total = total + received_ref[source]
        turned = total * cos_ref[...] + pltpu.roll(total, HD // 2, 1) * sin_ref[...]
        turned = turned.astype(jnp.bfloat16)
        for target in range(pool_size):
            out_ref[target] = turned

    return pl.pallas_call(
        body, out_shape=jax.ShapeDtypeStruct((pool_size, rows, HD), jnp.bfloat16), name="finish_rows",
        compiler_params=small_grant(4),
    )(received, cos_rows, sin_rows)


def attend(lengths, new_rows, rotated, values, local_heads, group_size):
    pool_size = new_rows.shape[0]
    all_items, slots, _ = rotated.shape
    my_count = all_items // pool_size
    pair = 2 if my_count % 2 == 0 else 1
    rows = pair * group_size
    query_rows = my_count * group_size
    scale = HD ** (-0.5)

    groups = [[first + k for k in range(pair)] for first in range(0, my_count, pair)]

    def body(lengths_ref, new_ref, key_hbm, value_hbm, out_ref, key_refs, value_refs, sems):
        def copies(block):
            span = pl.ds(block * my_count, my_count)
            return (
                pltpu.make_async_copy(key_hbm.at[span], key_refs.at[block], sems.at[0, block]),
                pltpu.make_async_copy(value_hbm.at[span], value_refs.at[block], sems.at[1, block]),
            )

        for block in range(pool_size):
            for copy in copies(block):
                copy.start()
        pool_index = lax.axis_index("pool")

        def step(block, carry):
            one_block(
                block, pool_index, copies(block), lengths_ref, new_ref, key_refs.at[block], value_refs.at[block], out_ref
            )
            return carry

        lax.fori_loop(0, pool_size, step, 0)

    def one_block(block, pool_index, copies, lengths_ref, new_ref, key_ref, value_ref, out_ref):
        row_index = lax.broadcasted_iota(jnp.int32, (rows, 1), 0)
        slot_index = lax.broadcasted_iota(jnp.int32, (query_rows, slots), 1)
        lane = lax.broadcasted_iota(jnp.int32, (rows, HD), 1)
        holds_own = pool_index == 0
        in_item = [row_index // group_size == k for k in range(pair)]

        def spread(piece, width):
            return jnp.concatenate(
                [jnp.broadcast_to(piece(item), (group_size, width)) for item in range(my_count)], 0
            )

        queries = new_ref[block, :query_rows, :].astype(jnp.float32)
        own_rows = new_ref[block, query_rows:, :].astype(jnp.float32)
        for copy in copies:
            copy.wait()
        scores = []
        for index, items in enumerate(groups):
            part = queries[index * rows : (index + 1) * rows]
            wide_queries = jnp.concatenate([jnp.where(mask, part, 0.0).astype(jnp.bfloat16) for mask in in_item], 1)
            wide_keys = jnp.concatenate([key_ref[item] for item in items], 1)
            scores.append(
                lax.dot_general(
                    wide_queries, wide_keys, (((1,), (1,)), ((), ())), preferred_element_type=jnp.float32
                )
            )
        scores = jnp.concatenate(scores, 0) * scale
        limits = spread(lambda item: jnp.full((1, 1), lengths_ref[(block * my_count + item) // local_heads]), 1)
        valid = slot_index + pool_index * slots < limits
        scores = jnp.where(valid, scores, NEG)
        own_keys = spread(lambda item: own_rows[item : item + 1], HD)
        own_values = spread(lambda item: own_rows[my_count + item : my_count + item + 1], HD)
        own_score = jnp.sum(queries * own_keys, 1, keepdims=True) * scale
        own_score = jnp.where(holds_own, own_score, NEG)
        peak = jnp.maximum(jnp.max(scores, 1, keepdims=True), own_score)
        weights = jnp.where(valid, jnp.exp(scores - peak), 0.0)
        own_weight = jnp.where(holds_own, jnp.exp(own_score - peak), 0.0)
        total = jnp.sum(weights, 1, keepdims=True) + own_weight
        coarse = weights.astype(jnp.bfloat16)
        fine = (weights - coarse.astype(jnp.float32)).astype(jnp.bfloat16)
        blended = []
        for index, items in enumerate(groups):
            span = slice(index * rows, (index + 1) * rows)
            wide_values = jnp.concatenate([value_ref[item] for item in items], 1)
            both = jnp.dot(
                jnp.concatenate([coarse[span], fine[span]], 0), wide_values, preferred_element_type=jnp.float32
            )
            both = both[:rows] + both[rows:]
            chosen = both[:, :HD]
            for k in range(1, pair):
                chosen = jnp.where(in_item[k], both[:, k * HD : (k + 1) * HD], chosen)
            blended.append(chosen)
        blended = jnp.concatenate(blended, 0) + own_weight * own_values
        safe_total = jnp.maximum(total, 1e-30)
        out_ref[block, :query_rows, :] = (blended / safe_total).astype(jnp.bfloat16)
        level = jnp.where(total > 0, peak + jnp.log(safe_total), NEG)
        stamp = jnp.zeros((rows, HD), jnp.float32)
        for part in range(3):
            rounded = level.astype(jnp.bfloat16).astype(jnp.float32)
            level = level - rounded
            for index in range(len(groups)):
                stamp = jnp.where(lane == index * 3 + part, rounded[index * rows : (index + 1) * rows], stamp)
        out_ref[block, query_rows:, :] = stamp.astype(jnp.bfloat16)

    vmem = pl.BlockSpec(memory_space=pltpu.VMEM)
    hbm = pl.BlockSpec(memory_space=pltpu.HBM)
    cache_shape = (pool_size, my_count, slots, HD)
    return pl.pallas_call(
        body,
        in_specs=[pl.BlockSpec(memory_space=pltpu.SMEM), vmem, hbm, hbm],
        out_specs=vmem,
        out_shape=jax.ShapeDtypeStruct((pool_size, query_rows + rows, HD), jnp.bfloat16),
        scratch_shapes=[
            pltpu.VMEM(cache_shape, rotated.dtype),
            pltpu.VMEM(cache_shape, values.dtype),
            pltpu.SemaphoreType.DMA((2, pool_size)),
        ],
        compiler_params=small_grant(53),
        name="attend",
    )(lengths, new_rows, rotated, values)


def combine(parts, my_count, group_size):
    pool_size = parts.shape[0]
    pair = 2 if my_count % 2 == 0 else 1
    rows = pair * group_size
    query_rows = my_count * group_size

    def body(parts_ref, out_ref):
        lane = lax.broadcasted_iota(jnp.int32, (rows, HD), 1)
        stamps = [parts_ref[source, query_rows:, :].astype(jnp.float32) for source in range(pool_size)]
        for group in range(my_count // pair):
            in_group = (lane >= group * 3) & (lane < group * 3 + 3)
            levels = [jnp.sum(jnp.where(in_group, stamp, 0.0), 1, keepdims=True) for stamp in stamps]
            top = levels[0]
            for level in levels[1:]:
                top = jnp.maximum(top, level)
            factors = [jnp.exp(level - top) for level in levels]
            whole = factors[0]
            for factor in factors[1:]:
                whole = whole + factor
            span = slice(group * rows, (group + 1) * rows)
            blended = jnp.zeros((rows, HD), jnp.float32)
            for source in range(pool_size):
                blended = blended + parts_ref[source, span, :].astype(jnp.float32) * factors[source]
            blended = (blended / whole).astype(jnp.bfloat16)
            for target in range(pool_size):
                out_ref[target, span, :] = blended

    return pl.pallas_call(
        body, out_shape=jax.ShapeDtypeStruct((pool_size, query_rows, HD), jnp.bfloat16), name="combine",
        compiler_params=small_grant(4),
    )(parts)


def feed_forward(state, gate_weight, up_weight, down_weight):
    pool_size, prompts, block_cols = state.shape
    width = pool_size * block_cols
    hidden = gate_weight.shape[1]
    across = (((1,), (1,)), ((), ()))

    def body(state_ref, gate_hbm, up_hbm, down_hbm, out_ref, gate_ref, up_ref, down_ref, sems):
        spans = [slice(k * block_cols, (k + 1) * block_cols) for k in range(pool_size)]
        copies = []
        for index, span in enumerate(spans):
            for which, (source, target) in enumerate(((gate_hbm, gate_ref), (up_hbm, up_ref), (down_hbm, down_ref))):
                copies.append(pltpu.make_async_copy(source.at[:, span], target.at[:, span], sems.at[which, index]))
        for index in range(pool_size):
            copies[3 * index].start()
            copies[3 * index + 1].start()
        for index in range(pool_size):
            copies[3 * index + 2].start()
        squares = jnp.zeros((prompts, 1), jnp.float32)
        for source in range(pool_size):
            rows = state_ref[source].astype(jnp.float32)
            squares = squares + jnp.sum(rows * rows, 1, keepdims=True)
        inverse = lax.rsqrt(squares / width + EPS)
        gate_values = jnp.zeros((prompts, hidden), jnp.float32)
        up_values = jnp.zeros((prompts, hidden), jnp.float32)
        for index, span in enumerate(spans):
            rows = (state_ref[index].astype(jnp.float32) * inverse).astype(jnp.bfloat16)
            copies[3 * index].wait()
            gate_values = gate_values + lax.dot_general(
                rows, gate_ref[:, span], across, preferred_element_type=jnp.float32
            )
            copies[3 * index + 1].wait()
            up_values = up_values + lax.dot_general(
                rows, up_ref[:, span], across, preferred_element_type=jnp.float32
            )
        active = (gate_values / (1.0 + jnp.exp(-gate_values)) * up_values).astype(jnp.bfloat16)
        for index, span in enumerate(spans):
            copies[3 * index + 2].wait()
            out_ref[index] = jnp.dot(active, down_ref[:, span], preferred_element_type=jnp.float32).astype(
                jnp.bfloat16
            )

    whole = pl.BlockSpec(memory_space=pltpu.VMEM)
    return pl.pallas_call(
        body,
        in_specs=[whole] + [pl.BlockSpec(memory_space=pltpu.HBM)] * 3,
        scratch_shapes=[
            pltpu.VMEM((hidden, width), gate_weight.dtype),
            pltpu.VMEM((hidden, width), up_weight.dtype),
            pltpu.VMEM((hidden, width), down_weight.dtype),
            pltpu.SemaphoreType.DMA((3, pool_size)),
        ],
        out_shape=jax.ShapeDtypeStruct(state.shape, jnp.bfloat16),
        name="feed_forward",
        compiler_params=small_grant(48),
        cost_estimate=pl.CostEstimate(
            flops=6 * prompts * width * hidden, bytes_accessed=6 * width * hidden, transcendentals=prompts * hidden
        ),
    )(state, gate_weight.T, up_weight.T, down_weight)


def exchange(pieces):
    return lax.all_to_all(pieces, "pool", 0, 0, tiled=True)


def gather(block):
    pool_size = lax.axis_size("pool")
    return exchange(jnp.broadcast_to(block[None], (pool_size,) + block.shape))


def heads_sum(values):
    size = lax.axis_size("heads")
    total = values
    moved = values
    for _ in range(size - 1):
        moved = lax.ppermute(moved, "heads", [(k, (k + 1) % size) for k in range(size)])
        total = total + moved
    return total


def per_device(
    hidden_in,
    key_cache,
    value_cache,
    positions,
    query_pos,
    lengths,
    query_weight,
    key_weight,
    value_weight,
    out_weight,
    gate_weight,
    up_weight,
    down_weight,
):
    pool_index = lax.axis_index("pool")
    pool_size = lax.axis_size("pool")
    prompts, width = hidden_in.shape
    local_heads, seq_local = key_cache.shape[1:3]
    query_width = query_weight.shape[1] // local_heads
    group_size = query_width // HD
    all_items = prompts * local_heads
    my_count = all_items // pool_size
    my_start = pool_index * my_count
    block_cols = width // pool_size

    weights = (query_weight, key_weight, value_weight)
    received = exchange(project(hidden_in, weights, pool_size, local_heads, group_size))

    pairs = prompts // 2
    early = (5 * pairs) // 8
    paired_keys = key_cache.reshape((2, pairs) + key_cache.shape[1:])
    rotated = rope_keys(paired_keys, positions, 0, early, None)
    value_rows = value_cache.reshape(all_items, seq_local, HD)
    row_items = my_start + jnp.concatenate(
        [jnp.repeat(jnp.arange(my_count), group_size), jnp.arange(my_count), jnp.arange(my_count)]
    )
    row_prompts = row_items // local_heads
    turning = (jnp.arange(my_count * (group_size + 2)) < my_count * (group_size + 1))[:, None]
    picked = (row_prompts[:, None] == jnp.arange(prompts)) & turning
    section = sections()
    chosen = jnp.zeros((row_items.shape[0], HD // 2), jnp.int32)
    for axis in range(3):
        ids = jnp.sum(jnp.where(picked, query_pos[axis][None], 0), 1)
        chosen = jnp.where(section == axis, ids[:, None], chosen)
    sine, cosine = sin_cos(chosen.astype(jnp.float32) * frequencies())
    cos_rows = jnp.concatenate([cosine, cosine], 1)
    sin_rows = jnp.concatenate([-sine, sine], 1)
    received, rotated = lax.optimization_barrier((received, rotated))
    finished, rotated = lax.optimization_barrier((finish_rows(received, cos_rows, sin_rows), rotated))
    new_rows = exchange(finished)
    rotated = rope_keys(paired_keys, positions, early, pairs, rotated).reshape(all_items, seq_local, HD)

    parts = exchange(attend(lengths, new_rows, rotated, value_rows, local_heads, group_size))
    attended = exchange(combine(parts, my_count, group_size))
    attn_out = heads_sum(project_out(attended, out_weight, prompts))
    hidden_cols = lax.dynamic_slice_in_dim(hidden_in, pool_index * block_cols, block_cols, 1)
    mid_state = (hidden_cols.astype(jnp.float32) + attn_out).astype(jnp.bfloat16)
    pieces = exchange(feed_forward(gather(mid_state), gate_weight, up_weight, down_weight))
    mlp_cols = heads_sum(jnp.sum(pieces.astype(jnp.float32), 0))
    return (mid_state.astype(jnp.float32) + mlp_cols).astype(jnp.bfloat16)


def solution(mesh):
    in_specs = (
        P("groups", None),
        P("groups", "heads", "pool", None),
        P("groups", "heads", "pool", None),
        P(None, "groups", "pool"),
        P(None, "groups"),
        P("groups"),
        P("pool", "heads"),
        P("pool", "heads"),
        P("pool", "heads"),
        P("heads", "pool"),
        P(None, ("pool", "heads")),
        P(None, ("pool", "heads")),
        P(("pool", "heads"), None),
    )
    out_specs = P("groups", "pool")
    return jax.shard_map(per_device, mesh=mesh, in_specs=in_specs, out_specs=out_specs, check_vma=False)
```

```python
import math

import jax
import jax.numpy as jnp
from jax import lax
from jax.experimental import pallas as pl
from jax.experimental.pallas import tpu as pltpu
from jax.sharding import PartitionSpec as P

HD = 128
EPS = 1e-06
THETA = 1000000.0
NEG = -1e30


def sin_cos(angles):
    turns = (angles * (2.0 / math.pi) + 0.5).astype(jnp.int32)
    count = turns.astype(jnp.float32)
    rest = angles - count * 1.5703125
    rest = rest - count * 4.837512969970703125e-4
    rest = rest - count * 7.54978995489188216e-8
    square = rest * rest
    sine = ((-1.9515295891e-4 * square + 8.3321608736e-3) * square - 1.6666654611e-1) * square * rest + rest
    cosine = ((2.443315711809948e-5 * square - 1.388731625493765e-3) * square + 4.166664568298827e-2) * square
    cosine = (cosine - 0.5) * square + 1.0
    odd = (turns & 1) == 1
    sin_out = jnp.where(odd, cosine, sine)
    cos_out = jnp.where(odd, sine, cosine)
    sin_out = jnp.where((turns & 2) == 2, -sin_out, sin_out)
    cos_out = jnp.where(((turns + 1) & 2) == 2, -cos_out, cos_out)
    return sin_out, cos_out


def frequencies():
    column = jnp.arange(HD // 2)
    return jnp.exp(column.astype(jnp.float32) * (-2.0 * math.log(THETA) / HD))


def sections():
    first_end = HD // 8
    second_end = first_end + 3 * HD // 16
    column = jnp.arange(HD // 2)
    return (column >= first_end).astype(jnp.int32) + (column >= second_end).astype(jnp.int32)


def in_hbm(array):
    return pltpu.with_memory_space_constraint(array, pltpu.HBM)


def small_grant(mebibytes):
    return pltpu.CompilerParams(vmem_limit_bytes=mebibytes << 20)


def rope_keys(key_cache, positions, first_pair, last_pair, partner):
    _, pairs, heads, slots, _ = key_cache.shape
    low_bits = 6
    chunk = min(slots, 64)
    count = last_pair - first_pair
    inverse = jnp.tile(frequencies(), 2)[None]

    def body(positions_ref, inverse_ref, key_hbm, *refs):
        out_hbm, key_ref, out_ref, chosen_ref, cos_ref, sin_ref, sems = refs[-7:]

        def copy_in(index):
            return pltpu.make_async_copy(key_hbm.at[:, first_pair + index], key_ref.at[:, index], sems.at[0, index])

        def copy_out(index):
            return pltpu.make_async_copy(out_ref.at[:, index], out_hbm.at[:, first_pair + index], sems.at[1, index])

        for index in range(count):
            copy_in(index).start()
        first = lax.broadcasted_iota(jnp.int32, (chunk, HD), 1) < HD // 2
        row = lax.broadcasted_iota(jnp.int32, (16, HD), 0)
        lane = lax.broadcasted_iota(jnp.int32, (16, HD), 1)
        column = lane % (HD // 2)
        first_end = HD // 8
        section = (column >= first_end).astype(jnp.int32) + (column >= first_end + 3 * HD // 16).astype(jnp.int32)
        within = row % 8
        own_half = row // 8 == lane // (HD // 2)
        picker = jnp.where(own_half & (within == section), float(1 << low_bits), 0.0)
        picker = jnp.where(own_half & (within == section + 3), 1.0, picker).astype(jnp.bfloat16)
        blank = jnp.zeros((2, slots), jnp.float32)

        def step(index, carry):
            digits = []
            for half in range(2):
                ids = [positions_ref[axis, pl.ds(half * pairs + first_pair + index, 1), :] for axis in range(3)]
                digits += [(value >> low_bits).astype(jnp.float32) for value in ids]
                digits += [(value & ((1 << low_bits) - 1)).astype(jnp.float32) for value in ids]
                digits.append(blank)
            chosen_ref[...] = lax.dot_general(
                jnp.concatenate(digits, 0).astype(jnp.bfloat16),
                picker,
                (((0,), (0,)), ((), ())),
                preferred_element_type=jnp.float32,
            )
            for start in range(0, slots, chunk):
                rows = slice(start, start + chunk)
                sine, cosine = sin_cos(chosen_ref[rows, :] * inverse_ref[...])
                cosine_rolled = pltpu.roll(cosine, HD // 2, 1)
                sine_rolled = pltpu.roll(sine, HD // 2, 1)
                cos_ref[0, rows, :] = jnp.where(first, cosine, cosine_rolled)
                cos_ref[1, rows, :] = jnp.where(first, cosine_rolled, cosine)
                sin_ref[0, rows, :] = jnp.where(first, -sine, sine_rolled)
                sin_ref[1, rows, :] = jnp.where(first, -sine_rolled, sine)
            copy_in(index).wait()
            for half in range(2):
                for start in range(0, slots, chunk):
                    rows = slice(start, start + chunk)
                    cos_rows = cos_ref[half, rows, :]
                    sin_rows = sin_ref[half, rows, :]
                    for head in range(heads):
                        keys = key_ref[half, index, head, rows, :].astype(jnp.float32)
                        turned = keys * cos_rows + pltpu.roll(keys, HD // 2, 1) * sin_rows
                        out_ref[half, index, head, rows, :] = turned.astype(jnp.bfloat16)
            copy_out(index).start()
            return carry

        lax.fori_loop(0, count, step, 0)
        for index in range(count):
            copy_out(index).wait()

    vmem = pl.BlockSpec(memory_space=pltpu.VMEM)
    hbm = pl.BlockSpec(memory_space=pltpu.HBM)
    partners = () if partner is None else (partner,)
    return pl.pallas_call(
        body,
        in_specs=[vmem, vmem, hbm] + [hbm for _ in partners],
        out_specs=hbm,
        out_shape=jax.ShapeDtypeStruct(key_cache.shape, jnp.bfloat16),
        input_output_aliases={3: 0} if partners else {},
        scratch_shapes=[
            pltpu.VMEM((2, count) + key_cache.shape[2:], jnp.bfloat16),
            pltpu.VMEM((2, count) + key_cache.shape[2:], jnp.bfloat16),
            pltpu.VMEM((slots, HD), jnp.float32),
            pltpu.VMEM((2, slots, HD), jnp.float32),
            pltpu.VMEM((2, slots, HD), jnp.float32),
            pltpu.SemaphoreType.DMA((2, count)),
        ],
        compiler_params=small_grant(56),
        name="rope_keys",
    )(positions, inverse, key_cache, *partners)


def project(hidden_in, weights, pool_size, local_heads, group_size):
    prompts, width = hidden_in.shape
    block_cols = width // pool_size
    my_count = prompts * local_heads // pool_size
    rows = my_count * (group_size + 2)
    columns = [weight.shape[1] for weight in weights]
    query_columns = columns[0]
    pieces = max(1, min(8, query_columns // 512))
    piece = query_columns // pieces

    def place(kind, head, group):
        if kind == 0:
            return lambda item: item * group_size + group
        return lambda item: my_count * (group_size + kind - 1) + item

    def body(hidden_hbm, query_hbm, key_hbm, value_hbm, out_ref, query_ref, key_ref, value_ref, flat_ref, hidden_ref, sems):
        hidden_copy = pltpu.make_async_copy(hidden_hbm, hidden_ref, sems.at[pieces + 2])
        hidden_copy.start()
        copies = []
        for index in range(pieces):
            span = slice(index * piece, (index + 1) * piece)
            copies.append(pltpu.make_async_copy(query_hbm.at[:, span], query_ref.at[:, span], sems.at[index]))
        copies.append(pltpu.make_async_copy(key_hbm, key_ref, sems.at[pieces]))
        copies.append(pltpu.make_async_copy(value_hbm, value_ref, sems.at[pieces + 1]))
        for copy in copies:
            copy.start()
        hidden_copy.wait()
        hidden = hidden_ref[...].astype(jnp.float32)
        squares = jnp.sum(hidden * hidden, 1, keepdims=True)
        start = pl.multiple_of(lax.axis_index("pool") * block_cols, block_cols)
        mine = hidden_ref[:, pl.ds(start, block_cols)].astype(jnp.float32)
        normed = (mine * lax.rsqrt(squares / width + EPS)).astype(jnp.bfloat16)

        def spread(kind, first_block, count, values):
            for offset in range(count):
                flat_ref[offset * prompts : (offset + 1) * prompts, :] = values[:, offset * HD : (offset + 1) * HD]
                number = first_block + offset
                head, group = (number // group_size, number % group_size) if kind == 0 else (number, 0)
                row_of = place(kind, head, group)
                if my_count >= local_heads:
                    per_device = my_count // local_heads
                    for turn in range(per_device):
                        out_ref[pl.ds(row_of(turn * local_heads + head), pool_size, stride=rows), :] = flat_ref[
                            pl.ds(offset * prompts + turn, pool_size, stride=per_device), :
                        ]
                else:
                    split = local_heads // my_count
                    base = (head // my_count) * rows + row_of(head % my_count)
                    out_ref[pl.ds(base, prompts, stride=split * rows), :] = flat_ref[
                        offset * prompts : (offset + 1) * prompts, :
                    ]

        for index in range(pieces):
            span = slice(index * piece, (index + 1) * piece)
            copies[index].wait()
            values = jnp.dot(normed, query_ref[:, span], preferred_element_type=jnp.float32)
            spread(0, index * (piece // HD), piece // HD, values)
        for kind, ref in ((1, key_ref), (2, value_ref)):
            copies[pieces + kind - 1].wait()
            values = jnp.dot(normed, ref[...], preferred_element_type=jnp.float32)
            spread(kind, 0, local_heads, values)

    vmem = pl.BlockSpec(memory_space=pltpu.VMEM)
    hbm = pl.BlockSpec(memory_space=pltpu.HBM)
    out = pl.pallas_call(
        body,
        in_specs=[hbm, hbm, hbm, hbm],
        out_specs=vmem,
        out_shape=jax.ShapeDtypeStruct((pool_size * rows, HD), jnp.float32),
        scratch_shapes=[pltpu.VMEM(weight.shape, weight.dtype) for weight in weights]
        + [
            pltpu.VMEM((prompts * max(piece // HD, local_heads), HD), jnp.float32),
            pltpu.VMEM(hidden_in.shape, hidden_in.dtype),
            pltpu.SemaphoreType.DMA((pieces + 3,)),
        ],
        compiler_params=small_grant(56),
        name="project",
    )(in_hbm(hidden_in), *[in_hbm(weight) for weight in weights])
    return out.reshape(pool_size, rows, HD)


def project_out(attended, out_weight, prompts):
    total_rows = attended.shape[0] * attended.shape[1]
    blocks = total_rows // prompts
    attended = attended.reshape(total_rows, HD)
    pieces = max(1, min(8, blocks // 2))
    per_piece = blocks // pieces
    depth = per_piece * HD

    def body(attended_ref, weight_hbm, out_ref, weight_ref, wide_ref, sems):
        copies = []
        for index in range(pieces):
            span = slice(index * depth, (index + 1) * depth)
            copies.append(pltpu.make_async_copy(weight_hbm.at[span], weight_ref.at[span], sems.at[index]))
            copies[-1].start()
        wide_ref[...] = attended_ref[...].astype(jnp.float32)
        total = jnp.zeros(out_ref.shape, jnp.float32)
        for index in range(pieces):
            rows = [
                wide_ref[pl.ds(index * per_piece + k, prompts, stride=blocks), :].astype(jnp.bfloat16)
                for k in range(per_piece)
            ]
            copies[index].wait()
            total = total + jnp.dot(
                jnp.concatenate(rows, 1),
                weight_ref[index * depth : (index + 1) * depth, :],
                preferred_element_type=jnp.float32,
            )
        out_ref[...] = total

    vmem = pl.BlockSpec(memory_space=pltpu.VMEM)
    return pl.pallas_call(
        body,
        in_specs=[vmem, pl.BlockSpec(memory_space=pltpu.HBM)],
        out_specs=vmem,
        out_shape=jax.ShapeDtypeStruct((prompts, out_weight.shape[1]), jnp.float32),
        scratch_shapes=[
            pltpu.VMEM(out_weight.shape, out_weight.dtype),
            pltpu.VMEM((total_rows, HD), jnp.float32),
            pltpu.SemaphoreType.DMA((pieces,)),
        ],
        compiler_params=small_grant(53),
        name="project_out",
    )(attended, out_weight)


def finish_rows(received, cos_rows, sin_rows):
    pool_size, rows, _ = received.shape

    def body(received_ref, cos_ref, sin_ref, out_ref):
        total = received_ref[0]
        for source in range(1, pool_size):
            total = total + received_ref[source]
        turned = total * cos_ref[...] + pltpu.roll(total, HD // 2, 1) * sin_ref[...]
        turned = turned.astype(jnp.bfloat16)
        for target in range(pool_size):
            out_ref[target] = turned

    return pl.pallas_call(
        body, out_shape=jax.ShapeDtypeStruct((pool_size, rows, HD), jnp.bfloat16), name="finish_rows",
        compiler_params=small_grant(4),
    )(received, cos_rows, sin_rows)


def attend(lengths, new_rows, rotated, values, local_heads, group_size):
    pool_size = new_rows.shape[0]
    all_items, slots, _ = rotated.shape
    my_count = all_items // pool_size
    pair = 2 if my_count % 2 == 0 else 1
    rows = pair * group_size
    query_rows = my_count * group_size
    scale = HD ** (-0.5)

    groups = [[first + k for k in range(pair)] for first in range(0, my_count, pair)]

    def body(lengths_ref, new_ref, key_hbm, value_hbm, out_ref, key_refs, value_refs, sems):
        def copies(block):
            span = pl.ds(block * my_count, my_count)
            return (
                pltpu.make_async_copy(key_hbm.at[span], key_refs.at[block], sems.at[0, block]),
                pltpu.make_async_copy(value_hbm.at[span], value_refs.at[block], sems.at[1, block]),
            )

        for block in range(pool_size):
            for copy in copies(block):
                copy.start()
        pool_index = lax.axis_index("pool")

        def step(block, carry):
            one_block(
                block, pool_index, copies(block), lengths_ref, new_ref, key_refs.at[block], value_refs.at[block], out_ref
            )
            return carry

        lax.fori_loop(0, pool_size, step, 0)

    def one_block(block, pool_index, copies, lengths_ref, new_ref, key_ref, value_ref, out_ref):
        row_index = lax.broadcasted_iota(jnp.int32, (rows, 1), 0)
        slot_index = lax.broadcasted_iota(jnp.int32, (query_rows, slots), 1)
        lane = lax.broadcasted_iota(jnp.int32, (rows, HD), 1)
        holds_own = pool_index == 0
        in_item = [row_index // group_size == k for k in range(pair)]

        def spread(piece, width):
            return jnp.concatenate(
                [jnp.broadcast_to(piece(item), (group_size, width)) for item in range(my_count)], 0
            )

        queries = new_ref[block, :query_rows, :].astype(jnp.float32)
        own_rows = new_ref[block, query_rows:, :].astype(jnp.float32)
        for copy in copies:
            copy.wait()
        scores = []
        for index, items in enumerate(groups):
            part = queries[index * rows : (index + 1) * rows]
            wide_queries = jnp.concatenate([jnp.where(mask, part, 0.0).astype(jnp.bfloat16) for mask in in_item], 1)
            wide_keys = jnp.concatenate([key_ref[item] for item in items], 1)
            scores.append(
                lax.dot_general(
                    wide_queries, wide_keys, (((1,), (1,)), ((), ())), preferred_element_type=jnp.float32
                )
            )
        scores = jnp.concatenate(scores, 0) * scale
        limits = spread(lambda item: jnp.full((1, 1), lengths_ref[(block * my_count + item) // local_heads]), 1)
        valid = slot_index + pool_index * slots < limits
        scores = jnp.where(valid, scores, NEG)
        own_keys = spread(lambda item: own_rows[item : item + 1], HD)
        own_values = spread(lambda item: own_rows[my_count + item : my_count + item + 1], HD)
        own_score = jnp.sum(queries * own_keys, 1, keepdims=True) * scale
        own_score = jnp.where(holds_own, own_score, NEG)
        peak = jnp.maximum(jnp.max(scores, 1, keepdims=True), own_score)
        weights = jnp.where(valid, jnp.exp(scores - peak), 0.0)
        own_weight = jnp.where(holds_own, jnp.exp(own_score - peak), 0.0)
        total = jnp.sum(weights, 1, keepdims=True) + own_weight
        coarse = weights.astype(jnp.bfloat16)
        fine = (weights - coarse.astype(jnp.float32)).astype(jnp.bfloat16)
        blended = []
        for index, items in enumerate(groups):
            span = slice(index * rows, (index + 1) * rows)
            wide_values = jnp.concatenate([value_ref[item] for item in items], 1)
            both = jnp.dot(
                jnp.concatenate([coarse[span], fine[span]], 0), wide_values, preferred_element_type=jnp.float32
            )
            both = both[:rows] + both[rows:]
            chosen = both[:, :HD]
            for k in range(1, pair):
                chosen = jnp.where(in_item[k], both[:, k * HD : (k + 1) * HD], chosen)
            blended.append(chosen)
        blended = jnp.concatenate(blended, 0) + own_weight * own_values
        safe_total = jnp.maximum(total, 1e-30)
        out_ref[block, :query_rows, :] = (blended / safe_total).astype(jnp.bfloat16)
        level = jnp.where(total > 0, peak + jnp.log(safe_total), NEG)
        stamp = jnp.zeros((rows, HD), jnp.float32)
        for part in range(3):
            rounded = level.astype(jnp.bfloat16).astype(jnp.float32)
            level = level - rounded
            for index in range(len(groups)):
                stamp = jnp.where(lane == index * 3 + part, rounded[index * rows : (index + 1) * rows], stamp)
        out_ref[block, query_rows:, :] = stamp.astype(jnp.bfloat16)

    vmem = pl.BlockSpec(memory_space=pltpu.VMEM)
    hbm = pl.BlockSpec(memory_space=pltpu.HBM)
    cache_shape = (pool_size, my_count, slots, HD)
    return pl.pallas_call(
        body,
        in_specs=[pl.BlockSpec(memory_space=pltpu.SMEM), vmem, hbm, hbm],
        out_specs=vmem,
        out_shape=jax.ShapeDtypeStruct((pool_size, query_rows + rows, HD), jnp.bfloat16),
        scratch_shapes=[
            pltpu.VMEM(cache_shape, rotated.dtype),
            pltpu.VMEM(cache_shape, values.dtype),
            pltpu.SemaphoreType.DMA((2, pool_size)),
        ],
        compiler_params=small_grant(53),
        name="attend",
    )(lengths, new_rows, rotated, values)


def combine(parts, my_count, group_size):
    pool_size = parts.shape[0]
    pair = 2 if my_count % 2 == 0 else 1
    rows = pair * group_size
    query_rows = my_count * group_size

    def body(parts_ref, out_ref):
        lane = lax.broadcasted_iota(jnp.int32, (rows, HD), 1)
        stamps = [parts_ref[source, query_rows:, :].astype(jnp.float32) for source in range(pool_size)]
        for group in range(my_count // pair):
            in_group = (lane >= group * 3) & (lane < group * 3 + 3)
            levels = [jnp.sum(jnp.where(in_group, stamp, 0.0), 1, keepdims=True) for stamp in stamps]
            top = levels[0]
            for level in levels[1:]:
                top = jnp.maximum(top, level)
            factors = [jnp.exp(level - top) for level in levels]
            whole = factors[0]
            for factor in factors[1:]:
                whole = whole + factor
            span = slice(group * rows, (group + 1) * rows)
            blended = jnp.zeros((rows, HD), jnp.float32)
            for source in range(pool_size):
                blended = blended + parts_ref[source, span, :].astype(jnp.float32) * factors[source]
            blended = (blended / whole).astype(jnp.bfloat16)
            for target in range(pool_size):
                out_ref[target, span, :] = blended

    return pl.pallas_call(
        body, out_shape=jax.ShapeDtypeStruct((pool_size, query_rows, HD), jnp.bfloat16), name="combine",
        compiler_params=small_grant(4),
    )(parts)


def gather_by_halves(block):
    pool_size = lax.axis_size("pool")

    def device(pool, core):
        return 2 * pool + core

    parts = []
    for turn in range(pool_size // 2):
        pairs = []
        for pool in range(pool_size):
            target = (pool + 2 * turn) % pool_size
            if turn:
                pairs.append((device(pool, 0), device(target, 0)))
            pairs.append((device(pool, 1), device(target ^ 1, 1)))
        parts.append(lax.ppermute(block, ("pool", "heads"), pairs))
    parts[0] = jnp.where(lax.axis_index("heads") == 0, block, parts[0])
    mine = jnp.stack(parts)
    return mine, lax.ppermute(mine, "heads", [(0, 1), (1, 0)])


def sources_by_halves(pool_size):
    pool = lax.axis_index("pool")
    core = lax.axis_index("heads")
    straight = [(pool + pool_size - 2 * turn) % pool_size for turn in range(pool_size // 2)]
    other = pool + 1 - 2 * (pool % 2)
    crossed = [(other + pool_size - 2 * turn) % pool_size for turn in range(pool_size // 2)]
    mine = [jnp.where(core == 0, a, b) for a, b in zip(straight, crossed)]
    theirs = [jnp.where(core == 0, b, a) for a, b in zip(straight, crossed)]
    return mine + theirs


def feed_forward(states, gate_weight, up_weight, down_weight, pool_size):
    _, prompts, block_cols = states[0].shape
    width = pool_size * block_cols
    hidden = gate_weight.shape[0]
    across = (((1,), (1,)), ((), ()))

    def body(*refs):
        state_refs = refs[: len(states)]
        gate_hbm, up_hbm, down_hbm, out_ref, gate_ref, up_ref, down_ref, sems = refs[len(states) :]
        sources = list(range(pool_size)) if len(states) == 1 else sources_by_halves(pool_size)
        blocks = [(ref, index) for ref in state_refs for index in range(ref.shape[0])]
        copies = []
        spans = []
        for turn, source in enumerate(sources):
            start = source * block_cols
            if len(states) > 1:
                start = pl.multiple_of(start, block_cols)
            spans.append(pl.ds(start, block_cols))
            for which, (origin, held) in enumerate(((gate_hbm, gate_ref), (up_hbm, up_ref))):
                copies.append(
                    pltpu.make_async_copy(origin.at[:, spans[-1]], held.at[:, spans[-1]], sems.at[which, turn])
                )
                copies[-1].start()
        down_copies = []
        for index in range(pool_size):
            span = slice(index * block_cols, (index + 1) * block_cols)
            down_copies.append(pltpu.make_async_copy(down_hbm.at[:, span], down_ref.at[:, span], sems.at[2, index]))
            down_copies[-1].start()
        squares = jnp.zeros((prompts, 1), jnp.float32)
        for ref, index in blocks:
            rows = ref[index].astype(jnp.float32)
            squares = squares + jnp.sum(rows * rows, 1, keepdims=True)
        inverse = lax.rsqrt(squares / width + EPS)
        gate_values = jnp.zeros((prompts, hidden), jnp.float32)
        up_values = jnp.zeros((prompts, hidden), jnp.float32)
        normed = []
        for (ref, index), span in zip(blocks, spans):
            normed.append((ref[index].astype(jnp.float32) * inverse).astype(jnp.bfloat16))
        for step in range(pool_size):
            copies[2 * step].wait()
            gate_values = gate_values + lax.dot_general(
                normed[step], gate_ref[:, spans[step]], across, preferred_element_type=jnp.float32
            )
            copies[2 * step + 1].wait()
            up_values = up_values + lax.dot_general(
                normed[step], up_ref[:, spans[step]], across, preferred_element_type=jnp.float32
            )
        active = (gate_values / (1.0 + jnp.exp(-gate_values)) * up_values).astype(jnp.bfloat16)
        for index in range(pool_size):
            span = slice(index * block_cols, (index + 1) * block_cols)
            down_copies[index].wait()
            out_ref[index] = jnp.dot(active, down_ref[:, span], preferred_element_type=jnp.float32).astype(
                jnp.bfloat16
            )

    whole = pl.BlockSpec(memory_space=pltpu.VMEM)
    hbm = pl.BlockSpec(memory_space=pltpu.HBM)
    return pl.pallas_call(
        body,
        in_specs=[whole] * len(states) + [hbm] * 3,
        out_shape=jax.ShapeDtypeStruct((pool_size, prompts, block_cols), jnp.bfloat16),
        scratch_shapes=[
            pltpu.VMEM((hidden, width), gate_weight.dtype),
            pltpu.VMEM((hidden, width), up_weight.dtype),
            pltpu.VMEM((hidden, width), down_weight.dtype),
            pltpu.SemaphoreType.DMA((3, pool_size)),
        ],
        name="feed_forward",
        compiler_params=small_grant(48),
        cost_estimate=pl.CostEstimate(
            flops=6 * prompts * width * hidden, bytes_accessed=6 * width * hidden, transcendentals=prompts * hidden
        ),
    )(*states, in_hbm(gate_weight), in_hbm(up_weight), in_hbm(down_weight))


def exchange(pieces):
    return lax.all_to_all(pieces, "pool", 0, 0, tiled=True)


def gather(block):
    pool_size = lax.axis_size("pool")
    return exchange(jnp.broadcast_to(block[None], (pool_size,) + block.shape))


def heads_sum(values):
    size = lax.axis_size("heads")
    total = values
    moved = values
    for _ in range(size - 1):
        moved = lax.ppermute(moved, "heads", [(k, (k + 1) % size) for k in range(size)])
        total = total + moved
    return total


def per_device(
    hidden_in,
    key_cache,
    value_cache,
    positions,
    query_pos,
    lengths,
    query_weight,
    key_weight,
    value_weight,
    out_weight,
    gate_weight,
    up_weight,
    down_weight,
):
    pool_index = lax.axis_index("pool")
    pool_size = lax.axis_size("pool")
    prompts, width = hidden_in.shape
    local_heads, seq_local = key_cache.shape[1:3]
    query_width = query_weight.shape[1] // local_heads
    group_size = query_width // HD
    all_items = prompts * local_heads
    my_count = all_items // pool_size
    my_start = pool_index * my_count
    block_cols = width // pool_size

    weights = (query_weight, key_weight, value_weight)
    received = exchange(project(hidden_in, weights, pool_size, local_heads, group_size))

    pairs = prompts // 2
    early = (6 * pairs) // 8
    paired_keys = key_cache.reshape((2, pairs) + key_cache.shape[1:])
    rotated = rope_keys(paired_keys, positions, 0, early, None)
    value_rows = value_cache.reshape(all_items, seq_local, HD)
    row_items = my_start + jnp.concatenate(
        [jnp.repeat(jnp.arange(my_count), group_size), jnp.arange(my_count), jnp.arange(my_count)]
    )
    row_prompts = row_items // local_heads
    turning = (jnp.arange(my_count * (group_size + 2)) < my_count * (group_size + 1))[:, None]
    picked = (row_prompts[:, None] == jnp.arange(prompts)) & turning
    section = sections()
    chosen = jnp.zeros((row_items.shape[0], HD // 2), jnp.int32)
    for axis in range(3):
        ids = jnp.sum(jnp.where(picked, query_pos[axis][None], 0), 1)
        chosen = jnp.where(section == axis, ids[:, None], chosen)
    sine, cosine = sin_cos(chosen.astype(jnp.float32) * frequencies())
    cos_rows = jnp.concatenate([cosine, cosine], 1)
    sin_rows = jnp.concatenate([-sine, sine], 1)
    received, rotated = lax.optimization_barrier((received, rotated))
    finished, rotated = lax.optimization_barrier((finish_rows(received, cos_rows, sin_rows), rotated))
    new_rows = exchange(finished)
    rotated = rope_keys(paired_keys, positions, early, pairs, rotated).reshape(all_items, seq_local, HD)

    parts = exchange(attend(lengths, new_rows, rotated, value_rows, local_heads, group_size))
    attended = exchange(combine(parts, my_count, group_size))
    attn_out = heads_sum(project_out(attended, out_weight, prompts))
    hidden_cols = lax.dynamic_slice_in_dim(hidden_in, pool_index * block_cols, block_cols, 1)
    mid_state = (hidden_cols.astype(jnp.float32) + attn_out).astype(jnp.bfloat16)
    if pool_size <= 8 and pool_size % 2 == 0 and lax.axis_size("heads") == 2:
        states = gather_by_halves(mid_state)
    else:
        states = (gather(mid_state),)
    pieces = exchange(feed_forward(states, gate_weight.T, up_weight.T, down_weight, pool_size))
    mlp_cols = heads_sum(jnp.sum(pieces.astype(jnp.float32), 0))
    return (mid_state.astype(jnp.float32) + mlp_cols).astype(jnp.bfloat16)


def solution(mesh):
    in_specs = (
        P("groups", None),
        P("groups", "heads", "pool", None),
        P("groups", "heads", "pool", None),
        P(None, "groups", "pool"),
        P(None, "groups"),
        P("groups"),
        P("pool", "heads"),
        P("pool", "heads"),
        P("pool", "heads"),
        P("heads", "pool"),
        P(None, ("pool", "heads")),
        P(None, ("pool", "heads")),
        P(("pool", "heads"), None),
    )
    out_specs = P("groups", "pool")
    return jax.shard_map(per_device, mesh=mesh, in_specs=in_specs, out_specs=out_specs, check_vma=False)
```

```python
import math

import jax
import jax.numpy as jnp
import numpy as np
from jax import lax
from jax.experimental import pallas as pl
from jax.experimental.pallas import tpu as pltpu
from jax.sharding import PartitionSpec as P

HD = 128
EPS = 1e-06
THETA = 1000000.0
NEG = -1e30


def sin_cos(angles):
    turns = (angles * (2.0 / math.pi) + 0.5).astype(jnp.int32)
    count = turns.astype(jnp.float32)
    rest = angles - count * 1.5703125
    rest = rest - count * 4.837512969970703125e-4
    rest = rest - count * 7.54978995489188216e-8
    square = rest * rest
    sine = ((-1.9515295891e-4 * square + 8.3321608736e-3) * square - 1.6666654611e-1) * square * rest + rest
    cosine = ((2.443315711809948e-5 * square - 1.388731625493765e-3) * square + 4.166664568298827e-2) * square
    cosine = (cosine - 0.5) * square + 1.0
    odd = (turns & 1) == 1
    sin_out = jnp.where(odd, cosine, sine)
    cos_out = jnp.where(odd, sine, cosine)
    sin_out = jnp.where((turns & 2) == 2, -sin_out, sin_out)
    cos_out = jnp.where(((turns + 1) & 2) == 2, -cos_out, cos_out)
    return sin_out, cos_out


def frequencies():
    column = np.arange(HD // 2, dtype=np.float32)
    exponents = column * np.float32(-2.0 * math.log(THETA) / HD)
    return np.exp(exponents.astype(np.float64)).astype(np.float32)


def sections():
    first_end = HD // 8
    second_end = first_end + 3 * HD // 16
    column = jnp.arange(HD // 2)
    return (column >= first_end).astype(jnp.int32) + (column >= second_end).astype(jnp.int32)


def in_hbm(array):
    return pltpu.with_memory_space_constraint(array, pltpu.HBM)


def small_grant(mebibytes):
    return pltpu.CompilerParams(vmem_limit_bytes=mebibytes << 20)


def rope_keys(key_cache, positions, first_pair, last_pair, partner):
    _, pairs, heads, slots, _ = key_cache.shape
    low_bits = 6
    chunk = min(slots, 64)
    count = last_pair - first_pair
    inverse = jnp.asarray(np.tile(frequencies(), 2)[None])

    def body(positions_ref, inverse_ref, key_hbm, *refs):
        out_hbm, key_ref, out_ref, chosen_ref, cos_ref, sin_ref, sems = refs[-7:]

        def copy_in(index):
            return pltpu.make_async_copy(key_hbm.at[:, first_pair + index], key_ref.at[:, index], sems.at[0, index])

        def copy_out(index):
            return pltpu.make_async_copy(out_ref.at[:, index], out_hbm.at[:, first_pair + index], sems.at[1, index])

        for index in range(count):
            copy_in(index).start()
        first = lax.broadcasted_iota(jnp.int32, (chunk, HD), 1) < HD // 2
        row = lax.broadcasted_iota(jnp.int32, (16, HD), 0)
        lane = lax.broadcasted_iota(jnp.int32, (16, HD), 1)
        column = lane % (HD // 2)
        first_end = HD // 8
        section = (column >= first_end).astype(jnp.int32) + (column >= first_end + 3 * HD // 16).astype(jnp.int32)
        within = row % 8
        own_half = row // 8 == lane // (HD // 2)
        picker = jnp.where(own_half & (within == section), float(1 << low_bits), 0.0)
        picker = jnp.where(own_half & (within == section + 3), 1.0, picker).astype(jnp.bfloat16)
        blank = jnp.zeros((2, slots), jnp.float32)

        def step(index, carry):
            digits = []
            for half in range(2):
                ids = [positions_ref[axis, pl.ds(half * pairs + first_pair + index, 1), :] for axis in range(3)]
                digits += [(value >> low_bits).astype(jnp.float32) for value in ids]
                digits += [(value & ((1 << low_bits) - 1)).astype(jnp.float32) for value in ids]
                digits.append(blank)
            chosen_ref[...] = lax.dot_general(
                jnp.concatenate(digits, 0).astype(jnp.bfloat16),
                picker,
                (((0,), (0,)), ((), ())),
                preferred_element_type=jnp.float32,
            )
            for start in range(0, slots, chunk):
                rows = slice(start, start + chunk)
                sine, cosine = sin_cos(chosen_ref[rows, :] * inverse_ref[...])
                cosine_rolled = pltpu.roll(cosine, HD // 2, 1)
                sine_rolled = pltpu.roll(sine, HD // 2, 1)
                cos_ref[0, rows, :] = jnp.where(first, cosine, cosine_rolled)
                cos_ref[1, rows, :] = jnp.where(first, cosine_rolled, cosine)
                sin_ref[0, rows, :] = jnp.where(first, -sine, sine_rolled)
                sin_ref[1, rows, :] = jnp.where(first, -sine_rolled, sine)
            copy_in(index).wait()
            for half in range(2):
                for start in range(0, slots, chunk):
                    rows = slice(start, start + chunk)
                    cos_rows = cos_ref[half, rows, :]
                    sin_rows = sin_ref[half, rows, :]
                    for head in range(heads):
                        keys = key_ref[half, index, head, rows, :].astype(jnp.float32)
                        turned = keys * cos_rows + pltpu.roll(keys, HD // 2, 1) * sin_rows
                        out_ref[half, index, head, rows, :] = turned.astype(jnp.bfloat16)
            copy_out(index).start()
            return carry

        lax.fori_loop(0, count, step, 0)
        for index in range(count):
            copy_out(index).wait()

    vmem = pl.BlockSpec(memory_space=pltpu.VMEM)
    hbm = pl.BlockSpec(memory_space=pltpu.HBM)
    partners = () if partner is None else (partner,)
    return pl.pallas_call(
        body,
        in_specs=[vmem, vmem, hbm] + [hbm for _ in partners],
        out_specs=hbm,
        out_shape=jax.ShapeDtypeStruct(key_cache.shape, jnp.bfloat16),
        input_output_aliases={3: 0} if partners else {},
        scratch_shapes=[
            pltpu.VMEM((2, count) + key_cache.shape[2:], jnp.bfloat16),
            pltpu.VMEM((2, count) + key_cache.shape[2:], jnp.bfloat16),
            pltpu.VMEM((slots, HD), jnp.float32),
            pltpu.VMEM((2, slots, HD), jnp.float32),
            pltpu.VMEM((2, slots, HD), jnp.float32),
            pltpu.SemaphoreType.DMA((2, count)),
        ],
        compiler_params=small_grant(56),
        name="rope_keys",
    )(positions, inverse, key_cache, *partners)


def project(hidden_in, weights, pool_size, local_heads, group_size):
    prompts, width = hidden_in.shape
    block_cols = width // pool_size
    my_count = prompts * local_heads // pool_size
    rows = my_count * (group_size + 2)
    columns = [weight.shape[1] for weight in weights]
    query_columns = columns[0]
    pieces = max(1, min(8, query_columns // 512))
    piece = query_columns // pieces

    def place(kind, head, group):
        if kind == 0:
            return lambda item: item * group_size + group
        return lambda item: my_count * (group_size + kind - 1) + item

    def body(hidden_hbm, query_hbm, key_hbm, value_hbm, out_ref, query_ref, key_ref, value_ref, flat_ref, hidden_ref, sems):
        hidden_copy = pltpu.make_async_copy(hidden_hbm, hidden_ref, sems.at[pieces + 2])
        hidden_copy.start()
        copies = []
        for index in range(pieces):
            span = slice(index * piece, (index + 1) * piece)
            copies.append(pltpu.make_async_copy(query_hbm.at[:, span], query_ref.at[:, span], sems.at[index]))
        copies.append(pltpu.make_async_copy(key_hbm, key_ref, sems.at[pieces]))
        copies.append(pltpu.make_async_copy(value_hbm, value_ref, sems.at[pieces + 1]))
        for copy in copies:
            copy.start()
        hidden_copy.wait()
        hidden = hidden_ref[...].astype(jnp.float32)
        squares = jnp.sum(hidden * hidden, 1, keepdims=True)
        start = pl.multiple_of(lax.axis_index("pool") * block_cols, block_cols)
        mine = hidden_ref[:, pl.ds(start, block_cols)].astype(jnp.float32)
        normed = (mine * lax.rsqrt(squares / width + EPS)).astype(jnp.bfloat16)

        def spread(kind, first_block, count, values):
            for offset in range(count):
                flat_ref[offset * prompts : (offset + 1) * prompts, :] = values[:, offset * HD : (offset + 1) * HD]
                number = first_block + offset
                head, group = (number // group_size, number % group_size) if kind == 0 else (number, 0)
                row_of = place(kind, head, group)
                if my_count >= local_heads:
                    per_device = my_count // local_heads
                    for turn in range(per_device):
                        out_ref[pl.ds(row_of(turn * local_heads + head), pool_size, stride=rows), :] = flat_ref[
                            pl.ds(offset * prompts + turn, pool_size, stride=per_device), :
                        ]
                else:
                    split = local_heads // my_count
                    base = (head // my_count) * rows + row_of(head % my_count)
                    out_ref[pl.ds(base, prompts, stride=split * rows), :] = flat_ref[
                        offset * prompts : (offset + 1) * prompts, :
                    ]

        for index in range(pieces):
            span = slice(index * piece, (index + 1) * piece)
            copies[index].wait()
            values = jnp.dot(normed, query_ref[:, span], preferred_element_type=jnp.float32)
            spread(0, index * (piece // HD), piece // HD, values)
        for kind, ref in ((1, key_ref), (2, value_ref)):
            copies[pieces + kind - 1].wait()
            values = jnp.dot(normed, ref[...], preferred_element_type=jnp.float32)
            spread(kind, 0, local_heads, values)

    vmem = pl.BlockSpec(memory_space=pltpu.VMEM)
    hbm = pl.BlockSpec(memory_space=pltpu.HBM)
    out = pl.pallas_call(
        body,
        in_specs=[hbm, hbm, hbm, hbm],
        out_specs=vmem,
        out_shape=jax.ShapeDtypeStruct((pool_size * rows, HD), jnp.float32),
        scratch_shapes=[pltpu.VMEM(weight.shape, weight.dtype) for weight in weights]
        + [
            pltpu.VMEM((prompts * max(piece // HD, local_heads), HD), jnp.float32),
            pltpu.VMEM(hidden_in.shape, hidden_in.dtype),
            pltpu.SemaphoreType.DMA((pieces + 3,)),
        ],
        compiler_params=small_grant(56),
        name="project",
    )(in_hbm(hidden_in), *[in_hbm(weight) for weight in weights])
    return out.reshape(pool_size, rows, HD)


def project_out(attended, out_weight, prompts):
    total_rows = attended.shape[0] * attended.shape[1]
    blocks = total_rows // prompts
    attended = attended.reshape(total_rows, HD)
    pieces = max(1, min(8, blocks // 2))
    per_piece = blocks // pieces
    depth = per_piece * HD

    def body(attended_ref, weight_hbm, out_ref, weight_ref, wide_ref, sems):
        copies = []
        for index in range(pieces):
            span = slice(index * depth, (index + 1) * depth)
            copies.append(pltpu.make_async_copy(weight_hbm.at[span], weight_ref.at[span], sems.at[index]))
            copies[-1].start()
        wide_ref[...] = attended_ref[...].astype(jnp.float32)
        total = jnp.zeros(out_ref.shape, jnp.float32)
        for index in range(pieces):
            rows = [
                wide_ref[pl.ds(index * per_piece + k, prompts, stride=blocks), :].astype(jnp.bfloat16)
                for k in range(per_piece)
            ]
            copies[index].wait()
            total = total + jnp.dot(
                jnp.concatenate(rows, 1),
                weight_ref[index * depth : (index + 1) * depth, :],
                preferred_element_type=jnp.float32,
            )
        out_ref[...] = total

    vmem = pl.BlockSpec(memory_space=pltpu.VMEM)
    return pl.pallas_call(
        body,
        in_specs=[vmem, pl.BlockSpec(memory_space=pltpu.HBM)],
        out_specs=vmem,
        out_shape=jax.ShapeDtypeStruct((prompts, out_weight.shape[1]), jnp.float32),
        scratch_shapes=[
            pltpu.VMEM(out_weight.shape, out_weight.dtype),
            pltpu.VMEM((total_rows, HD), jnp.float32),
            pltpu.SemaphoreType.DMA((pieces,)),
        ],
        compiler_params=small_grant(53),
        name="project_out",
    )(attended, out_weight)


def finish_rows(received, cos_rows, sin_rows):
    pool_size, rows, _ = received.shape

    def body(received_ref, cos_ref, sin_ref, out_ref):
        total = received_ref[0]
        for source in range(1, pool_size):
            total = total + received_ref[source]
        turned = total * cos_ref[...] + pltpu.roll(total, HD // 2, 1) * sin_ref[...]
        turned = turned.astype(jnp.bfloat16)
        for target in range(pool_size):
            out_ref[target] = turned

    return pl.pallas_call(
        body, out_shape=jax.ShapeDtypeStruct((pool_size, rows, HD), jnp.bfloat16), name="finish_rows",
        compiler_params=small_grant(4),
    )(received, cos_rows, sin_rows)


def attend(lengths, new_rows, rotated, values, local_heads, group_size):
    pool_size = new_rows.shape[0]
    all_items, slots, _ = rotated.shape
    my_count = all_items // pool_size
    pair = 2 if my_count % 2 == 0 else 1
    rows = pair * group_size
    query_rows = my_count * group_size
    scale = HD ** (-0.5)

    groups = [[first + k for k in range(pair)] for first in range(0, my_count, pair)]

    def body(lengths_ref, new_ref, key_hbm, value_hbm, out_ref, key_refs, value_refs, sems):
        def copies(block):
            span = pl.ds(block * my_count, my_count)
            return (
                pltpu.make_async_copy(key_hbm.at[span], key_refs.at[block], sems.at[0, block]),
                pltpu.make_async_copy(value_hbm.at[span], value_refs.at[block], sems.at[1, block]),
            )

        for block in range(pool_size):
            for copy in copies(block):
                copy.start()
        pool_index = lax.axis_index("pool")

        def step(block, carry):
            one_block(
                block, pool_index, copies(block), lengths_ref, new_ref, key_refs.at[block], value_refs.at[block], out_ref
            )
            return carry

        lax.fori_loop(0, pool_size, step, 0)

    def one_block(block, pool_index, copies, lengths_ref, new_ref, key_ref, value_ref, out_ref):
        row_index = lax.broadcasted_iota(jnp.int32, (rows, 1), 0)
        slot_index = lax.broadcasted_iota(jnp.int32, (query_rows, slots), 1)
        lane = lax.broadcasted_iota(jnp.int32, (rows, HD), 1)
        holds_own = pool_index == 0
        in_item = [row_index // group_size == k for k in range(pair)]

        def spread(piece, width):
            return jnp.concatenate(
                [jnp.broadcast_to(piece(item), (group_size, width)) for item in range(my_count)], 0
            )

        queries = new_ref[block, :query_rows, :].astype(jnp.float32)
        own_rows = new_ref[block, query_rows:, :].astype(jnp.float32)
        for copy in copies:
            copy.wait()
        scores = []
        for index, items in enumerate(groups):
            part = queries[index * rows : (index + 1) * rows]
            wide_queries = jnp.concatenate([jnp.where(mask, part, 0.0).astype(jnp.bfloat16) for mask in in_item], 1)
            wide_keys = jnp.concatenate([key_ref[item] for item in items], 1)
            scores.append(
                lax.dot_general(
                    wide_queries, wide_keys, (((1,), (1,)), ((), ())), preferred_element_type=jnp.float32
                )
            )
        scores = jnp.concatenate(scores, 0) * scale
        limits = spread(lambda item: jnp.full((1, 1), lengths_ref[(block * my_count + item) // local_heads]), 1)
        valid = slot_index + pool_index * slots < limits
        scores = jnp.where(valid, scores, NEG)
        own_keys = spread(lambda item: own_rows[item : item + 1], HD)
        own_values = spread(lambda item: own_rows[my_count + item : my_count + item + 1], HD)
        own_score = jnp.sum(queries * own_keys, 1, keepdims=True) * scale
        own_score = jnp.where(holds_own, own_score, NEG)
        peak = jnp.maximum(jnp.max(scores, 1, keepdims=True), own_score)
        weights = jnp.where(valid, jnp.exp(scores - peak), 0.0)
        own_weight = jnp.where(holds_own, jnp.exp(own_score - peak), 0.0)
        total = jnp.sum(weights, 1, keepdims=True) + own_weight
        coarse = weights.astype(jnp.bfloat16)
        fine = (weights - coarse.astype(jnp.float32)).astype(jnp.bfloat16)
        blended = []
        for index, items in enumerate(groups):
            span = slice(index * rows, (index + 1) * rows)
            wide_values = jnp.concatenate([value_ref[item] for item in items], 1)
            both = jnp.dot(
                jnp.concatenate([coarse[span], fine[span]], 0), wide_values, preferred_element_type=jnp.float32
            )
            both = both[:rows] + both[rows:]
            chosen = both[:, :HD]
            for k in range(1, pair):
                chosen = jnp.where(in_item[k], both[:, k * HD : (k + 1) * HD], chosen)
            blended.append(chosen)
        blended = jnp.concatenate(blended, 0) + own_weight * own_values
        safe_total = jnp.maximum(total, 1e-30)
        out_ref[block, :query_rows, :] = (blended / safe_total).astype(jnp.bfloat16)
        level = jnp.where(total > 0, peak + jnp.log(safe_total), NEG)
        stamp = jnp.zeros((rows, HD), jnp.float32)
        for part in range(3):
            rounded = level.astype(jnp.bfloat16).astype(jnp.float32)
            level = level - rounded
            for index in range(len(groups)):
                stamp = jnp.where(lane == index * 3 + part, rounded[index * rows : (index + 1) * rows], stamp)
        out_ref[block, query_rows:, :] = stamp.astype(jnp.bfloat16)

    vmem = pl.BlockSpec(memory_space=pltpu.VMEM)
    hbm = pl.BlockSpec(memory_space=pltpu.HBM)
    cache_shape = (pool_size, my_count, slots, HD)
    return pl.pallas_call(
        body,
        in_specs=[pl.BlockSpec(memory_space=pltpu.SMEM), vmem, hbm, hbm],
        out_specs=vmem,
        out_shape=jax.ShapeDtypeStruct((pool_size, query_rows + rows, HD), jnp.bfloat16),
        scratch_shapes=[
            pltpu.VMEM(cache_shape, rotated.dtype),
            pltpu.VMEM(cache_shape, values.dtype),
            pltpu.SemaphoreType.DMA((2, pool_size)),
        ],
        compiler_params=small_grant(53),
        name="attend",
    )(lengths, new_rows, rotated, values)


def combine(parts, my_count, group_size):
    pool_size = parts.shape[0]
    pair = 2 if my_count % 2 == 0 else 1
    rows = pair * group_size
    query_rows = my_count * group_size

    def body(parts_ref, out_ref):
        lane = lax.broadcasted_iota(jnp.int32, (rows, HD), 1)
        stamps = [parts_ref[source, query_rows:, :].astype(jnp.float32) for source in range(pool_size)]
        for group in range(my_count // pair):
            in_group = (lane >= group * 3) & (lane < group * 3 + 3)
            levels = [jnp.sum(jnp.where(in_group, stamp, 0.0), 1, keepdims=True) for stamp in stamps]
            top = levels[0]
            for level in levels[1:]:
                top = jnp.maximum(top, level)
            factors = [jnp.exp(level - top) for level in levels]
            whole = factors[0]
            for factor in factors[1:]:
                whole = whole + factor
            span = slice(group * rows, (group + 1) * rows)
            blended = jnp.zeros((rows, HD), jnp.float32)
            for source in range(pool_size):
                blended = blended + parts_ref[source, span, :].astype(jnp.float32) * factors[source]
            blended = (blended / whole).astype(jnp.bfloat16)
            for target in range(pool_size):
                out_ref[target, span, :] = blended

    return pl.pallas_call(
        body, out_shape=jax.ShapeDtypeStruct((pool_size, query_rows, HD), jnp.bfloat16), name="combine",
        compiler_params=small_grant(4),
    )(parts)


def gather_by_halves(block):
    pool_size = lax.axis_size("pool")

    def device(pool, core):
        return 2 * pool + core

    parts = []
    for turn in range(pool_size // 2):
        pairs = []
        for pool in range(pool_size):
            target = (pool + 2 * turn) % pool_size
            if turn:
                pairs.append((device(pool, 0), device(target, 0)))
            pairs.append((device(pool, 1), device(target ^ 1, 1)))
        parts.append(lax.ppermute(block, ("pool", "heads"), pairs))
    parts[0] = jnp.where(lax.axis_index("heads") == 0, block, parts[0])
    mine = jnp.stack(parts)
    return mine, lax.ppermute(mine, "heads", [(0, 1), (1, 0)])


def sources_by_halves(pool_size):
    pool = lax.axis_index("pool")
    core = lax.axis_index("heads")
    straight = [(pool + pool_size - 2 * turn) % pool_size for turn in range(pool_size // 2)]
    other = pool + 1 - 2 * (pool % 2)
    crossed = [(other + pool_size - 2 * turn) % pool_size for turn in range(pool_size // 2)]
    mine = [jnp.where(core == 0, a, b) for a, b in zip(straight, crossed)]
    theirs = [jnp.where(core == 0, b, a) for a, b in zip(straight, crossed)]
    return mine + theirs


def feed_forward(states, gate_weight, up_weight, down_weight, pool_size):
    _, prompts, block_cols = states[0].shape
    width = pool_size * block_cols
    hidden = gate_weight.shape[0]
    across = (((1,), (1,)), ((), ()))

    def body(*refs):
        state_refs = refs[: len(states)]
        gate_hbm, up_hbm, down_hbm, out_ref, gate_ref, up_ref, down_ref, sems = refs[len(states) :]
        sources = list(range(pool_size)) if len(states) == 1 else sources_by_halves(pool_size)
        blocks = [(ref, index) for ref in state_refs for index in range(ref.shape[0])]
        copies = []
        spans = []
        for turn, source in enumerate(sources):
            start = source * block_cols
            if len(states) > 1:
                start = pl.multiple_of(start, block_cols)
            spans.append(pl.ds(start, block_cols))
            for which, (origin, held) in enumerate(((gate_hbm, gate_ref), (up_hbm, up_ref))):
                copies.append(
                    pltpu.make_async_copy(origin.at[:, spans[-1]], held.at[:, spans[-1]], sems.at[which, turn])
                )
                copies[-1].start()
        down_copies = []
        for index in range(pool_size):
            span = slice(index * block_cols, (index + 1) * block_cols)
            down_copies.append(pltpu.make_async_copy(down_hbm.at[:, span], down_ref.at[:, span], sems.at[2, index]))
            down_copies[-1].start()
        squares = jnp.zeros((prompts, 1), jnp.float32)
        for ref, index in blocks:
            rows = ref[index].astype(jnp.float32)
            squares = squares + jnp.sum(rows * rows, 1, keepdims=True)
        inverse = lax.rsqrt(squares / width + EPS)
        gate_values = jnp.zeros((prompts, hidden), jnp.float32)
        up_values = jnp.zeros((prompts, hidden), jnp.float32)
        normed = []
        for (ref, index), span in zip(blocks, spans):
            normed.append((ref[index].astype(jnp.float32) * inverse).astype(jnp.bfloat16))
        for step in range(pool_size):
            copies[2 * step].wait()
            gate_values = gate_values + lax.dot_general(
                normed[step], gate_ref[:, spans[step]], across, preferred_element_type=jnp.float32
            )
            copies[2 * step + 1].wait()
            up_values = up_values + lax.dot_general(
                normed[step], up_ref[:, spans[step]], across, preferred_element_type=jnp.float32
            )
        active = (gate_values / (1.0 + jnp.exp(-gate_values)) * up_values).astype(jnp.bfloat16)
        for index in range(pool_size):
            span = slice(index * block_cols, (index + 1) * block_cols)
            down_copies[index].wait()
            out_ref[index] = jnp.dot(active, down_ref[:, span], preferred_element_type=jnp.float32).astype(
                jnp.bfloat16
            )

    whole = pl.BlockSpec(memory_space=pltpu.VMEM)
    hbm = pl.BlockSpec(memory_space=pltpu.HBM)
    return pl.pallas_call(
        body,
        in_specs=[whole] * len(states) + [hbm] * 3,
        out_shape=jax.ShapeDtypeStruct((pool_size, prompts, block_cols), jnp.bfloat16),
        scratch_shapes=[
            pltpu.VMEM((hidden, width), gate_weight.dtype),
            pltpu.VMEM((hidden, width), up_weight.dtype),
            pltpu.VMEM((hidden, width), down_weight.dtype),
            pltpu.SemaphoreType.DMA((3, pool_size)),
        ],
        name="feed_forward",
        compiler_params=small_grant(48),
        cost_estimate=pl.CostEstimate(
            flops=6 * prompts * width * hidden, bytes_accessed=6 * width * hidden, transcendentals=prompts * hidden
        ),
    )(*states, in_hbm(gate_weight), in_hbm(up_weight), in_hbm(down_weight))


def exchange(pieces):
    return lax.all_to_all(pieces, "pool", 0, 0, tiled=True)


def gather(block):
    pool_size = lax.axis_size("pool")
    return exchange(jnp.broadcast_to(block[None], (pool_size,) + block.shape))


def heads_sum(values):
    size = lax.axis_size("heads")
    total = values
    moved = values
    for _ in range(size - 1):
        moved = lax.ppermute(moved, "heads", [(k, (k + 1) % size) for k in range(size)])
        total = total + moved
    return total


def per_device(
    hidden_in,
    key_cache,
    value_cache,
    positions,
    query_pos,
    lengths,
    query_weight,
    key_weight,
    value_weight,
    out_weight,
    gate_weight,
    up_weight,
    down_weight,
):
    pool_index = lax.axis_index("pool")
    pool_size = lax.axis_size("pool")
    prompts, width = hidden_in.shape
    local_heads, seq_local = key_cache.shape[1:3]
    query_width = query_weight.shape[1] // local_heads
    group_size = query_width // HD
    all_items = prompts * local_heads
    my_count = all_items // pool_size
    my_start = pool_index * my_count
    block_cols = width // pool_size

    weights = (query_weight, key_weight, value_weight)
    received = exchange(project(hidden_in, weights, pool_size, local_heads, group_size))

    pairs = prompts // 2
    early = (6 * pairs) // 8
    paired_keys = key_cache.reshape((2, pairs) + key_cache.shape[1:])
    rotated = rope_keys(paired_keys, positions, 0, early, None)
    value_rows = value_cache.reshape(all_items, seq_local, HD)
    row_items = my_start + jnp.concatenate(
        [jnp.repeat(jnp.arange(my_count), group_size), jnp.arange(my_count), jnp.arange(my_count)]
    )
    row_prompts = row_items // local_heads
    turning = (jnp.arange(my_count * (group_size + 2)) < my_count * (group_size + 1))[:, None]
    picked = (row_prompts[:, None] == jnp.arange(prompts)) & turning
    section = sections()
    chosen = jnp.zeros((row_items.shape[0], HD // 2), jnp.int32)
    for axis in range(3):
        ids = jnp.sum(jnp.where(picked, query_pos[axis][None], 0), 1)
        chosen = jnp.where(section == axis, ids[:, None], chosen)
    sine, cosine = sin_cos(chosen.astype(jnp.float32) * frequencies())
    cos_rows = jnp.concatenate([cosine, cosine], 1)
    sin_rows = jnp.concatenate([-sine, sine], 1)
    received, rotated = lax.optimization_barrier((received, rotated))
    finished, rotated = lax.optimization_barrier((finish_rows(received, cos_rows, sin_rows), rotated))
    new_rows = exchange(finished)
    rotated = rope_keys(paired_keys, positions, early, pairs, rotated).reshape(all_items, seq_local, HD)

    parts = exchange(attend(lengths, new_rows, rotated, value_rows, local_heads, group_size))
    attended = exchange(combine(parts, my_count, group_size))
    attn_out = heads_sum(project_out(attended, out_weight, prompts))
    hidden_cols = lax.dynamic_slice_in_dim(hidden_in, pool_index * block_cols, block_cols, 1)
    mid_state = (hidden_cols.astype(jnp.float32) + attn_out).astype(jnp.bfloat16)
    if pool_size <= 8 and pool_size % 2 == 0 and lax.axis_size("heads") == 2:
        states = gather_by_halves(mid_state)
    else:
        states = (gather(mid_state),)
    pieces = exchange(feed_forward(states, gate_weight.T, up_weight.T, down_weight, pool_size))
    mlp_cols = heads_sum(jnp.sum(pieces.astype(jnp.float32), 0))
    return (mid_state.astype(jnp.float32) + mlp_cols).astype(jnp.bfloat16)


def solution(mesh):
    in_specs = (
        P("groups", None),
        P("groups", "heads", "pool", None),
        P("groups", "heads", "pool", None),
        P(None, "groups", "pool"),
        P(None, "groups"),
        P("groups"),
        P("pool", "heads"),
        P("pool", "heads"),
        P("pool", "heads"),
        P("heads", "pool"),
        P(None, ("pool", "heads")),
        P(None, ("pool", "heads")),
        P(("pool", "heads"), None),
    )
    out_specs = P("groups", "pool")
    return jax.shard_map(per_device, mesh=mesh, in_specs=in_specs, out_specs=out_specs, check_vma=False)
```
